768 devices in a mesh: gx: 12 (over z), gy: 4 (over x), gz: 16 (over y, core).
Axes of the slice: x: 4, y: 8, z: 12, core: 2. Of those that a mesh axis runs over, the one named last changes fastest.
Arguments:
- old_slots: bfloat16 [12, 4, 256, 4096], P('gx', 'gy', 'gz'), may hold values from -6 to 6
- old_ids: int32 [12, 4, 256], P('gx', 'gy', 'gz'), may hold values from -1 to 127, as said below
- old_owner: int32 [12, 4, 128], P('gx', 'gy'), may hold values from 0 to 15, as said below
- coefficient: float32 [192, 64, 2048], P('gx', 'gy', 'gz'), may hold values from 0.2 to 5
Outputs:
- solution: float32 [192, 64, 2048], P('gx', 'gy', 'gz')
The draws below stay inside these ranges and needn't reach their ends.
Inputs may be any that keep to these rules, and one draw needn't show every extreme that they name: old_owner[a, c, b] is the index along gz of the device that held box b of box column (a, c) before the move; no device holds more than 16 boxes of a column and some device holds exactly 16; no device holds more than 2 of the 8 boxes with one value of b // 8, and that bound is reached. old_ids[a, c, g * 16 + q] is the box held in slot q of device g of box column (a, c), or -1 for an empty slot; it agrees with old_owner and each box stands in exactly one slot.
All inputs are finite; a program needn't handle non-finite values.
Results may differ from the reference program's by a relative error of at most 0.0003.
Values may be sent and summed in bfloat16 or wider, within the bound.
A program may use at most 64 MiB of HBM per device.

```python
import math
import jax
import jax.numpy as jnp
from jax import lax

BOX = 16
NB = 8
SWEEPS = 2
CAP = 16
NX = 192
NY = 64
NZ = 2048
N_GX = 12
N_GY = 4
N_GZ = 16


def column_maps(column_key):
    groups = N_GZ
    halves = NB // 2
    pair_count = groups * halves
    subkeys = jax.random.split(column_key, 5)
    labels = jnp.arange(groups, dtype=jnp.int32)
    if NB <= groups:
        counts = jnp.where(labels < groups // 4, 2 * halves, jnp.where(labels < groups // 2, halves, halves // 2)).astype(jnp.int32)
    else:
        counts = jnp.full((groups,), halves, jnp.int32)
    ending = jnp.cumsum(counts).astype(jnp.int32)
    items = jnp.arange(pair_count, dtype=jnp.int32)
    sorted_owner = jnp.sum((items[:, None] >= ending[None, :]).astype(jnp.int32), axis=1)
    relabel = jax.random.permutation(subkeys[0], groups).astype(jnp.int32)
    item_owner = relabel[sorted_owner]
    columns = jax.random.permutation(subkeys[1], groups).astype(jnp.int32)
    target = columns[items % groups]
    levels = items // groups
    placing = jax.vmap(lambda single: jax.random.permutation(single, NB).astype(jnp.int32))(jax.random.split(subkeys[2], groups))
    first_box = target * NB + placing[target, 2 * levels]
    second_box = target * NB + placing[target, 2 * levels + 1]
    box_count = groups * NB
    owners = jnp.zeros((box_count,), jnp.int32).at[first_box].set(item_owner).at[second_box].set(item_owner)
    priority = jax.random.permutation(subkeys[3], box_count).astype(jnp.int32)
    sharing = owners[:, None] == owners[None, :]
    ranking = jnp.sum((sharing & (priority[None, :] < priority[:, None])).astype(jnp.int32), axis=1)
    offsets = jax.random.randint(subkeys[4], (groups,), 0, CAP, dtype=jnp.int32)
    slot_index = (ranking + offsets[owners]) % CAP
    slot_ids = jnp.full((groups * CAP,), -1, jnp.int32).at[owners * CAP + slot_index].set(jnp.arange(box_count, dtype=jnp.int32))
    return (owners, slot_ids)


def all_columns(key):
    column_keys = jax.random.split(jax.random.fold_in(key, 31), N_GX * N_GY)
    return jax.vmap(column_maps)(column_keys)


def draw_old_owner(key, part):
    owners, slot_ids = all_columns(key)
    return owners.reshape(N_GX, N_GY, N_GZ * NB)


def draw_old_ids(key, part):
    owners, slot_ids = all_columns(key)
    return slot_ids.reshape(N_GX, N_GY, N_GZ * CAP)


def draw_old_slots(key, part):
    shape = (N_GX, N_GY, N_GZ * CAP, BOX ** 3)
    noise_key = jax.random.fold_in(jax.random.fold_in(key, 47), 0)
    return jnp.clip(jax.random.normal(noise_key, shape, jnp.float32), -6.0, 6.0).astype(jnp.bfloat16)


def level_of(own_key, extent, cuts, low, largest):
    gain, own = 1.0, jax.random.fold_in(own_key, 6)
    for axis_at, shards_of in cuts:
        draws = jnp.exp(jax.random.uniform(jax.random.fold_in(own, axis_at), (shards_of,), jnp.float32, low / len(cuts), largest / len(cuts)))
        gain = gain * jnp.repeat(draws, extent[axis_at] // shards_of).reshape([-1 if axis == axis_at else 1 for axis in range(len(extent))])
    return gain


def setup_inputs(seed: int = 0) -> dict:
    key_list = jax.random.split(jax.random.key(seed), 5)
    return {
        "old_slots": draw_old_slots(jax.random.fold_in(key_list[4], 71), 0),
        "old_ids": draw_old_ids(jax.random.fold_in(key_list[4], 71), 0),
        "old_owner": draw_old_owner(jax.random.fold_in(key_list[4], 71), 0),
        "coefficient": jnp.clip(jnp.exp(math.log(5.0) - 3.218876 * jax.random.uniform(key_list[3], (NX, NY, NZ), jnp.float32) ** level_of(key_list[3], (NX, NY, NZ), ((0, 12), (1, 4), (2, 16)), -0.2, 0.2)), 0.2, 5.0),
    }


def inner(padded):
    return padded[1:-1, 1:-1, 1:-1]


def operator_parts(padded):
    face_first = 0.5 * (padded[:-1, 1:-1, 1:-1] + padded[1:, 1:-1, 1:-1])
    face_second = 0.5 * (padded[1:-1, :-1, 1:-1] + padded[1:-1, 1:, 1:-1])
    face_third = 0.5 * (padded[1:-1, 1:-1, :-1] + padded[1:-1, 1:-1, 1:])
    diagonal = face_first[:-1] + face_first[1:] + face_second[:, :-1] + face_second[:, 1:] + face_third[:, :, :-1] + face_third[:, :, 1:]
    return face_first, face_second, face_third, diagonal


def neighbours(padded, stencil):
    face_first, face_second, face_third, diagonal = stencil
    summed = face_first[:-1] * padded[:-2, 1:-1, 1:-1] + face_first[1:] * padded[2:, 1:-1, 1:-1]
    summed = summed + face_second[:, :-1] * padded[1:-1, :-2, 1:-1] + face_second[:, 1:] * padded[1:-1, 2:, 1:-1]
    summed = summed + face_third[:, :, :-1] * padded[1:-1, 1:-1, :-2] + face_third[:, :, 1:] * padded[1:-1, 1:-1, 2:]
    return summed


def red_cells(shape, margin):
    index_first = lax.broadcasted_iota(jnp.int32, shape, 0)
    index_second = lax.broadcasted_iota(jnp.int32, shape, 1)
    index_third = lax.broadcasted_iota(jnp.int32, shape, 2)
    return (index_first + index_second + index_third + margin) % 2 == 0


def relax(padded, source, stencil, factor, chosen):
    fresh = (factor * source + neighbours(padded, stencil)) / stencil[3]
    return jnp.where(chosen, fresh, inner(padded))


def apply_operator(values, stencil, factor):
    return (stencil[3] * values - neighbours(jnp.pad(values, 1), stencil)) / factor


def smooth(values, source, stencil, factor):
    red_mask = red_cells(source.shape, 0)
    black_mask = jnp.logical_not(red_mask)
    for counter in range(SWEEPS):
        values = relax(jnp.pad(values, 1), source, stencil, factor, red_mask)
        values = relax(jnp.pad(values, 1), source, stencil, factor, black_mask)
    return values


def coarsen(values):
    extent_first, extent_second, extent_third = values.shape
    grouped = values.reshape(extent_first // 2, 2, extent_second // 2, 2, extent_third // 2, 2)
    return grouped.mean(axis=(1, 3, 5))


def refine(values):
    return jnp.repeat(jnp.repeat(jnp.repeat(values, 2, axis=0), 2, axis=1), 2, axis=2)


def bicgstab(rhs_low, stencil, factor):
    image_low = apply_operator(rhs_low, stencil, factor)
    alpha_step = jnp.sum(rhs_low * rhs_low) / jnp.sum(rhs_low * image_low)
    rest_low = rhs_low - alpha_step * image_low
    turned = apply_operator(rest_low, stencil, factor)
    omega_step = jnp.sum(turned * rest_low) / jnp.sum(turned * turned)
    return alpha_step * rhs_low + omega_step * rest_low


def move_boxes(old_slots, old_ids, old_owner):
    column_boxes = NB * N_GZ
    held = old_ids.reshape(N_GX, N_GY, N_GZ, CAP)
    owner_index = jnp.broadcast_to(old_owner[:, :, :, None], (N_GX, N_GY, column_boxes, CAP))
    owner_slots = jnp.take_along_axis(held, owner_index, axis=2)
    wanted = jnp.arange(column_boxes, dtype=jnp.int32)
    position = jnp.argmax(owner_slots == wanted[None, None, :, None], axis=3).astype(jnp.int32)
    global_slot = old_owner * CAP + position
    picked = jax.vmap(jax.vmap(lambda stacked, chosen_rows: stacked[chosen_rows]))(old_slots, global_slot)
    boxes = picked.reshape(N_GX, N_GY, column_boxes, BOX, BOX, BOX).transpose(0, 3, 1, 4, 2, 5)
    return boxes.reshape(N_GX * BOX, N_GY * BOX, column_boxes * BOX)


def reference(old_slots, old_ids, old_owner, coefficient):
    source_fine = move_boxes(old_slots, old_ids, old_owner).astype(jnp.float32)
    stencil_fine = operator_parts(jnp.pad(coefficient, 1))
    fine_values = smooth(jnp.zeros_like(source_fine), source_fine, stencil_fine, 1.0)
    residual_fine = source_fine - apply_operator(fine_values, stencil_fine, 1.0)
    coefficient_mid = coarsen(coefficient)
    stencil_mid = operator_parts(jnp.pad(coefficient_mid, 1))
    source_mid = coarsen(residual_fine)
    middle_values = smooth(jnp.zeros_like(source_mid), source_mid, stencil_mid, 4.0)
    residual_mid = source_mid - apply_operator(middle_values, stencil_mid, 4.0)
    coefficient_low = coarsen(coefficient_mid)
    stencil_low = operator_parts(jnp.pad(coefficient_low, 1))
    bottom_values = bicgstab(coarsen(residual_mid), stencil_low, 16.0)
    middle_values = smooth(middle_values + refine(bottom_values), source_mid, stencil_mid, 4.0)
    return smooth(fine_values + refine(middle_values), source_fine, stencil_fine, 1.0)
```

```python
import functools

import jax
import jax.numpy as jnp
from jax import lax
from jax.experimental import pallas as pl
from jax.experimental.pallas import tpu as pltpu
from jax.sharding import PartitionSpec as P

BOX = 16
NB = 8
SEND = 2
LANES = 128
MESH = pl.DeviceIdType.MESH
F32 = jnp.float32
HI = lax.Precision.HIGHEST


def iota(shape, dim):
    return lax.broadcasted_iota(jnp.int32, shape, dim)


def place(axis, step):
    count = lax.axis_size(axis)
    return {axis: lax.rem(lax.axis_index(axis) + (step + count) % count, count)}


def remote(src, dst, send, recv, axis, step):
    return pltpu.make_async_remote_copy(
        src_ref=src,
        dst_ref=dst,
        send_sem=send,
        recv_sem=recv,
        device_id=place(axis, step),
        device_id_type=MESH,
    )


def edge_scale(axis, step):
    count = lax.axis_size(axis)
    at_edge = lax.axis_index(axis) == (0 if step < 0 else count - 1)
    return jnp.where(at_edge, 0.0, 1.0).astype(F32)


class Exchange:
    def __init__(self, send, recv, base):
        self.sems = [(send.at[base + i], recv.at[base + i]) for i in range(6)]
        self.flying = []

    def pair(self, at, axis, up_src, up_dst, down_src, down_dst):
        self.flying = [
            remote(up_src, up_dst, *self.sems[at], axis, 1),
            remote(down_src, down_dst, *self.sems[at + 1], axis, -1),
        ]
        for copy in self.flying:
            copy.start()

    def land(self):
        for copy in self.flying:
            copy.wait()


class Fine(Exchange):
    def __init__(self, array, packed, z_in, y_in, *sems):
        super().__init__(*sems)
        self.array, self.packed, self.z_in, self.y_in = array, packed, z_in, y_in

    def z_start(self):
        lane = iota((16, LANES), 1)
        packed = jnp.zeros((16, LANES), F32)
        for x in range(16):
            rolled = pltpu.roll(self.array[4 + x, 0:16, 0:LANES], (8 * x + 4) % LANES, 1)
            packed = jnp.where(lane // 8 == x, rolled, packed)
        self.packed[...] = packed
        self.pair(0, "gz", self.packed, self.z_in.at[0], self.packed, self.z_in.at[1])

    def z_finish(self, mask):
        self.land()
        lower, upper = self.z_in[0], self.z_in[1]
        if mask:
            lower, upper = lower * edge_scale("gz", -1), upper * edge_scale("gz", 1)
        both = jnp.where(iota((16, LANES), 1) % 8 < 4, lower, upper)
        for x in range(16):
            self.array[4 + x, 0:16, LANES:] = pltpu.roll(both, (2 * LANES - 8 * x - 4) % LANES, 1)

    def y_start(self):
        rows = self.array.at[pl.ds(4, 16)]
        self.pair(
            2,
            "gy",
            rows.at[:, pl.ds(8, 8), :],
            self.y_in.at[0],
            rows.at[:, pl.ds(0, 8), :],
            self.y_in.at[1],
        )

    def y_finish(self, mask):
        self.land()
        low_scale = edge_scale("gy", -1) if mask else None
        high_scale = edge_scale("gy", 1) if mask else None

        def body(x, _):
            lower, upper = self.y_in[0, x], self.y_in[1, x]
            if mask:
                lower, upper = lower * low_scale, upper * high_scale
            self.array[4 + x, 16:24, :] = jnp.where(iota((8, 256), 0) < 4, upper, lower)
            return 0

        lax.fori_loop(0, 16, body, 0)

    def x_start(self):
        a = self.array
        self.pair(
            4, "gx", a.at[pl.ds(16, 4)], a.at[pl.ds(0, 4)], a.at[pl.ds(4, 4)], a.at[pl.ds(20, 4)]
        )

    def x_finish(self, mask):
        self.land()
        if mask:
            self.array[0:4] = self.array[0:4] * edge_scale("gx", -1)
            self.array[20:24] = self.array[20:24] * edge_scale("gx", 1)


class Middle(Exchange):
    def __init__(self, array, z_in, *sems):
        super().__init__(*sems)
        self.array, self.z_in = array, z_in

    def z_start(self):
        own = self.array.at[pl.ds(6, 8), pl.ds(0, 8), :]
        self.pair(0, "gz", own, self.z_in.at[0], own, self.z_in.at[1])

    def z_finish(self, mask):
        self.land()
        lane = iota((8, LANES), 1)
        for x in range(8):
            lower, upper = self.z_in[0, x], self.z_in[1, x]
            if mask:
                lower, upper = lower * edge_scale("gz", -1), upper * edge_scale("gz", 1)
            halo = pltpu.roll(jnp.where(lane < 32, upper, lower), 64, 1)
            self.array[6 + x, 0:8, :] = jnp.where(lane < 64, self.array[6 + x, 0:8, :], halo)

    def y_start(self):
        rows = self.array.at[pl.ds(6, 8)]
        own = rows.at[:, pl.ds(0, 8), :]
        self.pair(2, "gy", own, rows.at[:, pl.ds(16, 8), :], own, rows.at[:, pl.ds(8, 8), :])

    def y_finish(self, mask):
        self.land()
        if mask:
            self.array[6:14, 16:24, :] = self.array[6:14, 16:24, :] * edge_scale("gy", -1)
            self.array[6:14, 8:16, :] = self.array[6:14, 8:16, :] * edge_scale("gy", 1)

    def x_start(self):
        a = self.array
        self.pair(
            4, "gx", a.at[pl.ds(8, 6)], a.at[pl.ds(0, 6)], a.at[pl.ds(6, 6)], a.at[pl.ds(14, 6)]
        )

    def x_finish(self, mask):
        self.land()
        if mask:
            self.array[0:6] = self.array[0:6] * edge_scale("gx", -1)
            self.array[14:20] = self.array[14:20] * edge_scale("gx", 1)


class Low(Exchange):
    def __init__(self, array, z_in, y_in, *sems):
        super().__init__(*sems)
        self.array, self.z_in, self.y_in = array, z_in, y_in

    def z_start(self):
        own = self.array.at[pl.ds(4, 4), pl.ds(0, 8), :]
        self.pair(0, "gz", own, self.z_in.at[0], own, self.z_in.at[1])

    def z_finish(self, mask):
        self.land()
        lane = iota((8, LANES), 1)
        for x in range(4):
            lower, upper = self.z_in[0, x], self.z_in[1, x]
            if mask:
                lower, upper = lower * edge_scale("gz", -1), upper * edge_scale("gz", 1)
            halo = jnp.where(lane < 64, pltpu.roll(upper, 32, 1), pltpu.roll(lower, 96, 1))
            self.array[4 + x, 0:8, :] = jnp.where(lane < 32, self.array[4 + x, 0:8, :], halo)

    def y_start(self):
        own = self.array.at[pl.ds(4, 4), pl.ds(0, 8), :]
        self.pair(2, "gy", own, self.y_in.at[0], own, self.y_in.at[1])

    def y_finish(self, mask):
        self.land()
        sub = iota((8, LANES), 0)
        for x in range(4):
            lower, upper = self.y_in[0, x], self.y_in[1, x]
            if mask:
                lower, upper = lower * edge_scale("gy", -1), upper * edge_scale("gy", 1)
            own = self.array[4 + x, 0:8, :]
            self.array[4 + x, 0:8, :] = jnp.where(sub < 4, own, pltpu.roll(upper, 4, 0))
            self.array[4 + x, 8:16, :] = pltpu.roll(lower, 4, 0)

    def x_start(self):
        a = self.array
        self.pair(
            4, "gx", a.at[pl.ds(4, 4)], a.at[pl.ds(0, 4)], a.at[pl.ds(4, 4)], a.at[pl.ds(8, 4)]
        )

    def x_finish(self, mask):
        self.land()
        if mask:
            self.array[0:4] = self.array[0:4] * edge_scale("gx", -1)
            self.array[8:12] = self.array[8:12] * edge_scale("gx", 1)


def exchange_all(exchanges, mask):
    for name in ("z", "y", "x"):
        for exchange in exchanges:
            getattr(exchange, name + "_start")()
        for exchange in exchanges:
            getattr(exchange, name + "_finish")(mask)


def make_stencil(kappa, scaled, diagonal, inverse):
    planes, rows, lanes = kappa.shape

    def body(x, _):
        here = kappa[x]
        around = (
            kappa[x - 1],
            kappa[x + 1],
            pltpu.roll(here, 1, 0),
            pltpu.roll(here, rows - 1, 0),
            pltpu.roll(here, 1, 1),
            pltpu.roll(here, lanes - 1, 1),
        )
        faces = [0.5 * (here + other) for other in around]
        total = faces[0] + faces[1] + faces[2] + faces[3] + faces[4] + faces[5]
        inside = here > 0.0
        inv = jnp.where(inside, 1.0 / total, 0.0)
        diagonal[x] = jnp.where(inside, total, 0.0)
        inverse[x] = inv
        for at in range(6):
            scaled[at, x] = faces[at] * inv
        return 0

    lax.fori_loop(1, planes - 1, body, 0)


def around_sum(scaled, values, x, rows, lanes):
    here = values[x]
    total = scaled[0, x] * values[x - 1] + scaled[1, x] * values[x + 1]
    total += scaled[2, x] * pltpu.roll(here, 1, 0)
    total += scaled[3, x] * pltpu.roll(here, rows - 1, 0)
    total += scaled[4, x] * pltpu.roll(here, 1, 1)
    total += scaled[5, x] * pltpu.roll(here, lanes - 1, 1)
    return here, total


def half_sweep(scaled, low, high, colour, pairs):
    rows, lanes = scaled.shape[2:]

    def body(x, _):
        chosen = (iota((rows, lanes), 0) + iota((rows, lanes), 1) + x) % 2 == colour
        for values, source in pairs:
            here, total = around_sum(scaled, values, x, rows, lanes)
            if source is not None:
                total += source[x]
            values[x] = jnp.where(chosen, total, here)
        return 0

    lax.fori_loop(low, high, body, 0)


def first_red(values, source, kappa):
    planes, rows, lanes = values.shape

    def body(x, _):
        red = (iota((rows, lanes), 0) + iota((rows, lanes), 1) + x) % 2 == 0
        kept = jnp.where(kappa[x] > 0.0, source[x], 0.0)
        source[x] = kept
        values[x] = jnp.where(red, kept, 0.0)
        return 0

    lax.fori_loop(0, planes, body, 0)


def pair_matrix():
    return jnp.where(iota((LANES, LANES), 0) // 2 == iota((LANES, LANES), 1), 1.0, 0.0).astype(F32)


def coarsen(planes, shelf):
    count = planes.shape[0] // 2
    rows = planes.shape[1]
    halves = planes.reshape(count, 2, rows, LANES)
    summed = halves[:, 0] + halves[:, 1]
    shelf[0:count, 0:rows, :] = summed
    if rows == 8:
        shelf[0:count, 8:16, :] = jnp.zeros((count, 8, LANES), F32)
    even = shelf[0:count, pl.ds(0, 8, stride=2), :]
    odd = shelf[0:count, pl.ds(1, 8, stride=2), :]
    flat = (even + odd).reshape(count * 8, LANES)
    out = jnp.dot(flat, pair_matrix(), precision=HI, preferred_element_type=F32)
    return 0.125 * out.reshape(count, 8, LANES)


def refine_low(values, shelf, target):
    coarse, lane = iota((LANES, LANES), 0), iota((LANES, LANES), 1)
    wanted = jnp.where(lane < 96, lane // 2, 64 + lane // 2)
    matrix = jnp.where(coarse == wanted, 1.0, 0.0).astype(F32)
    flat = values.reshape(12 * 16, LANES)
    wide = jnp.dot(flat, matrix, precision=HI, preferred_element_type=F32).reshape(12, 16, LANES)
    for x in range(12):
        for odd in range(2):
            shelf[x, pl.ds(odd, 8, stride=2), :] = wide[x, 0:8]
            shelf[x, pl.ds(16 + odd, 4, stride=2), :] = wide[x, 12:16]
    for x in range(20):
        target[x] = shelf[(x + 2) // 2]


def refine_middle(values, narrow, shelf, target, added, kappa):
    coarse, lane = iota((LANES, 2 * LANES), 0), iota((LANES, 2 * LANES), 1)
    matrix = jnp.where(coarse == lane // 2, 1.0, 0.0).astype(F32)
    sub = iota((8, LANES), 0)
    for x in range(12):
        narrow[x, 0:8, :] = values[4 + x, 0:8, :]
        tail = jnp.where(sub < 2, values[4 + x, 8:16, :], pltpu.roll(values[4 + x, 16:24, :], 4, 0))
        narrow[x, 8:16, :] = tail
    flat = narrow[...].reshape(12 * 16, LANES)
    wide = jnp.dot(flat, matrix, precision=HI, preferred_element_type=F32).reshape(12, 16, 256)
    for x in range(12):
        for half in range(2):
            part = wide[x, :, half * LANES : (half + 1) * LANES]
            for odd in range(2):
                shelf[half, x, pl.ds(odd, 8, stride=2), :] = part[0:8]
                shelf[half, x, pl.ds(16 + odd, 4, stride=2), :] = part[8:12]
    for x in range(24):
        for half in range(2):
            lanes = slice(half * LANES, (half + 1) * LANES)
            fresh = shelf[half, x // 2]
            if added is not None:
                fresh = jnp.where(kappa[x, :, lanes] > 0.0, fresh + added[x, :, lanes], 0.0)
            target[x, :, lanes] = fresh


def pack_boxes(slots, ids, stage, boxes, outgoing):
    for piece in range(32):
        stage[piece * 16 : (piece + 1) * 16, :] = slots[
            0, 0, :, piece * LANES : (piece + 1) * LANES
        ].astype(F32)
    for slot in range(16):
        boxes[slot] = stage[pl.ds(slot, 32, stride=16), :].astype(jnp.bfloat16)
    held = [ids[0, 0, slot] for slot in range(16)]
    targets = [lax.shift_right_arithmetic(box, 3) for box in held]
    keys = [box * 16 + slot for slot, box in enumerate(held)]

    def body(group, _):
        least, most = jnp.int32(1 << 20), jnp.int32(0)
        for target, key in zip(targets, keys):
            here = target == group
            least = jnp.where(here, jnp.minimum(least, key), least)
            most = jnp.where(here, jnp.maximum(most, key), most)
        outgoing[2 * group] = boxes[jnp.bitwise_and(least, 15)]
        outgoing[2 * group + 1] = boxes[jnp.bitwise_and(most, 15)]
        return 0

    lax.fori_loop(0, outgoing.shape[0] // SEND, body, 0)


def unpack_boxes(incoming, owner, shelf, source):
    me = lax.axis_index("gz")
    owners = [owner[0, 0, me * NB + at] for at in range(NB)]
    planes = []
    for at in range(NB):
        rank = jnp.int32(0)
        for before in range(at):
            rank = jnp.where(owners[before] == owners[at], 1, rank)
        planes.append(incoming[owners[at] * SEND + rank].astype(F32))
    group = iota((32, LANES), 1) // BOX
    for row in range(8):
        merged = jnp.zeros((32, LANES), F32)
        for at in range(NB):
            rolled = pltpu.roll(planes[at], (BOX * (at - row)) % LANES, 1)
            merged = jnp.where(group == at, rolled, merged)
        shelf[row * 32 : (row + 1) * 32, :] = merged
    for x in range(16):
        for half in range(2):
            source[x, half * 8 : half * 8 + 8, :] = shelf[pl.ds(2 * x + half, 8, stride=32), :]


class AllSum:
    def __init__(self, axis, out, into, send, recv, base):
        self.axis, self.out, self.into = axis, out, into
        self.count = lax.axis_size(axis)
        self.send, self.recv, self.base = send, recv, base

    def start(self, tile):
        self.out[...] = tile
        self.flying = []
        for step in range(1, self.count):
            sems = (self.send.at[self.base + step], self.recv.at[self.base + step])
            copy = remote(self.out, self.into.at[step], *sems, self.axis, step)
            copy.start()
            self.flying.append(copy)

    def finish(self):
        for copy in self.flying:
            copy.wait()
        total = self.out[...]
        for step in range(1, self.count):
            total += self.into[step]
        return total


def kernel(
    slots,
    ids,
    owner,
    coefficient,
    out,
    stage,
    boxes,
    outgoing,
    incoming,
    box_shelf,
    source,
    kap0,
    kap1,
    kap2,
    sc0,
    sc1,
    sc2,
    dia0,
    dia1,
    dia2,
    inv0,
    inv1,
    inv2,
    g0,
    u0,
    w0,
    g1,
    u1,
    w1,
    f2,
    p2,
    v2,
    b1,
    c1,
    b0,
    c0,
    shelf_c,
    shelf_r1,
    narrow,
    shelf_r0,
    packed,
    z0_in,
    y0_in,
    z1_in,
    z2_in,
    y2_in,
    sum_out,
    sum_y,
    sum_z,
    sum_x,
    send,
    recv,
    box_send,
    box_recv,
    sum_send,
    sum_recv,
):
    groups = lax.axis_size("gz")
    barrier = pltpu.get_barrier_semaphore()
    partners = 0
    for axis in ("gz", "gy", "gx"):
        for step in range(1, lax.axis_size(axis)):
            pl.semaphore_signal(barrier, inc=1, device_id=place(axis, step), device_id_type=MESH)
            partners += 1

    kap0[4:20, 0:16, 0:LANES] = coefficient[...]
    mid = coarsen(coefficient[...], shelf_c)
    kap1[6:14, 0:8, :] = mid
    kap2[4:8, 0:8, :] = coarsen(mid, shelf_c)
    pack_boxes(slots, ids, stage, boxes, outgoing)

    pl.semaphore_wait(barrier, partners)

    ex_k0 = Fine(kap0, packed.at[0], z0_in.at[0], y0_in.at[0], send, recv, 0)
    ex_k1 = Middle(kap1, z1_in.at[0], send, recv, 6)
    ex_k2 = Low(kap2, z2_in.at[0], y2_in.at[0], send, recv, 12)
    kappas = (ex_k0, ex_k1, ex_k2)
    for exchange in kappas:
        exchange.z_start()

    me = lax.axis_index("gz")
    moves = []
    for step in range(1, groups):
        there = place("gz", step)["gz"]
        copy = remote(
            outgoing.at[pl.ds(SEND * there, SEND)],
            incoming.at[pl.ds(SEND * me, SEND)],
            box_send.at[step],
            box_recv.at[step],
            "gz",
            step,
        )
        copy.start()
        moves.append(copy)
    incoming[pl.ds(SEND * me, SEND)] = outgoing[pl.ds(SEND * me, SEND)]

    for exchange in kappas:
        exchange.z_finish(True)
    for name in ("y", "x"):
        for exchange in kappas:
            getattr(exchange, name + "_start")()
        for exchange in kappas:
            getattr(exchange, name + "_finish")(True)

    make_stencil(kap0, sc0, dia0, inv0)
    make_stencil(kap1, sc1, dia1, inv1)
    make_stencil(kap2, sc2, dia2, inv2)

    for copy in moves:
        copy.wait()
    unpack_boxes(incoming, owner, box_shelf, source)

    g0[4:20, 0:16, 0:LANES] = source[...] * inv0[4:20, 0:16, 0:LANES]
    exchange_all((Fine(g0, packed.at[1], z0_in.at[1], y0_in.at[1], send, recv, 18),), False)
    first_red(u0, g0, kap0)
    half_sweep(sc0, 1, 23, 1, ((u0, g0),))
    half_sweep(sc0, 2, 22, 0, ((u0, g0),))
    half_sweep(sc0, 3, 21, 1, ((u0, g0),))
    w0[4:20, 0:16, 0:LANES] = u0[4:20, 0:16, 0:LANES]

    def residual(x, _):
        here, total = around_sum(sc0, u0, x + 4, 24, 256)
        rest = dia0[x + 4] * (g0[x + 4] + total - here)
        source[x] = rest[0:16, 0:LANES]
        return 0

    lax.fori_loop(0, 16, residual, 0)

    g1[6:14, 0:8, :] = 4.0 * coarsen(source[...], shelf_c) * inv1[6:14, 0:8, :]
    ex_g1 = Middle(g1, z1_in.at[1], send, recv, 24)
    ex_w0 = Fine(w0, packed.at[2], z0_in.at[2], y0_in.at[2], send, recv, 30)
    ex_g1.z_start()
    ex_w0.z_start()
    ex_g1.z_finish(False)
    ex_g1.y_start()
    ex_w0.z_finish(False)
    ex_g1.y_finish(False)
    ex_g1.x_start()
    ex_w0.y_start()
    ex_g1.x_finish(False)
    first_red(u1, g1, kap1)
    half_sweep(sc1, 1, 19, 1, ((u1, g1),))
    half_sweep(sc1, 2, 18, 0, ((u1, g1),))
    half_sweep(sc1, 3, 17, 1, ((u1, g1),))
    w1[6:14, 0:8, :] = u1[6:14, 0:8, :]

    rests = []
    for x in range(6, 14):
        here, total = around_sum(sc1, u1, x, 24, LANES)
        rest = (0.25 * dia1[x]) * (g1[x] + total - here)
        rests.append(rest[0:8])
    f2[4:8, 0:8, :] = coarsen(jnp.stack(rests), shelf_c)
    ex_f2 = Low(f2, z2_in.at[1], y2_in.at[1], send, recv, 36)
    ex_w1 = Middle(w1, z1_in.at[2], send, recv, 42)
    ex_f2.z_start()
    ex_w1.z_start()
    ex_w0.y_finish(False)
    ex_f2.z_finish(False)
    ex_f2.y_start()
    ex_w1.z_finish(False)
    ex_w1.y_start()
    ex_f2.y_finish(False)
    ex_f2.x_start()
    ex_w0.x_start()
    ex_f2.x_finish(False)
    p2[...] = jnp.where(kap2[...] > 0.0, f2[...], 0.0)

    v2[0] = jnp.zeros((16, LANES), F32)
    v2[11] = jnp.zeros((16, LANES), F32)
    for x in range(1, 11):
        here, total = around_sum(sc2, p2, x, 16, LANES)
        v2[x] = (0.0625 * dia2[x]) * (here - total)
    own = jnp.logical_and(iota((8, LANES), 0) < 4, iota((8, LANES), 1) < 32)
    sums = [jnp.zeros((8, LANES), F32) for _ in range(6)]
    for x in range(4, 8):
        image, total = around_sum(sc2, v2, x, 16, LANES)
        second = ((0.0625 * dia2[x]) * (image - total))[0:8]
        image, here = image[0:8], p2[x, 0:8, :]
        products = (
            here * here,
            here * image,
            image * image,
            second * here,
            second * image,
            second * second,
        )
        sums = [total + jnp.where(own, product, 0.0) for total, product in zip(sums, products)]
    tile = jnp.zeros((8, LANES), F32)
    for at in range(6):
        line = jnp.sum(sums[at], axis=0, keepdims=True)
        tile = jnp.where(iota((8, LANES), 0) == at, line, tile)

    sum_gy = AllSum("gy", sum_out.at[0], sum_y, sum_send, sum_recv, 0)
    sum_gz = AllSum("gz", sum_out.at[1], sum_z, sum_send, sum_recv, lax.axis_size("gy"))
    sum_gx = AllSum(
        "gx", sum_out.at[2], sum_x, sum_send, sum_recv, lax.axis_size("gy") + groups
    )
    sum_gy.start(tile)
    ex_w1.y_finish(False)
    ex_w1.x_start()

    refine_low(p2[...], shelf_r1, b1)
    refine_low(v2[...], shelf_r1, c1)
    ex_w1.x_finish(False)
    sum_gz.start(sum_gy.finish())
    u1[...] = jnp.where(kap1[...] > 0.0, w1[...], 0.0)
    triple = ((u1, g1), (b1, None), (c1, None))
    half_sweep(sc1, 1, 19, 0, triple)
    half_sweep(sc1, 2, 18, 1, triple)
    half_sweep(sc1, 3, 17, 0, triple)
    half_sweep(sc1, 4, 16, 1, triple)

    ex_w0.x_finish(False)
    refine_middle(u1, narrow, shelf_r0, u0, w0, kap0)
    sum_gx.start(sum_gz.finish())
    refine_middle(b1, narrow, shelf_r0, b0, None, None)
    refine_middle(c1, narrow, shelf_r0, c0, None, None)
    triple = ((u0, g0), (b0, None), (c0, None))
    half_sweep(sc0, 1, 23, 0, triple)
    half_sweep(sc0, 2, 22, 1, triple)
    half_sweep(sc0, 3, 21, 0, triple)
    half_sweep(sc0, 4, 20, 1, triple)

    totals = jnp.sum(sum_gx.finish(), axis=1, keepdims=True)
    norm_rhs, along, norm_image, second_rhs, second_along, norm_second = (
        totals[at : at + 1, :] for at in range(6)
    )
    alpha = norm_rhs / along
    turned_rest = along - alpha * norm_image - alpha * second_rhs + alpha * alpha * second_along
    turned_norm = norm_image - 2.0 * alpha * second_along + alpha * alpha * norm_second
    omega = turned_rest / turned_norm
    first = jnp.broadcast_to(alpha + omega, (16, LANES))
    other = jnp.broadcast_to(alpha * omega, (16, LANES))

    def combine(x, _):
        at = (x + 4, slice(0, 16), slice(0, LANES))
        out[x] = u0[at] + first * b0[at] - other * c0[at]
        return 0

    lax.fori_loop(0, 16, combine, 0)


def solution(mesh):
    sizes = dict(mesh.shape)

    def per_device(old_slots, old_ids, old_owner, coefficient):
        vmem = pl.BlockSpec(memory_space=pltpu.VMEM)
        smem = pl.BlockSpec(memory_space=pltpu.SMEM)
        fine, middle, low = (24, 24, 256), (20, 24, 128), (12, 16, 128)
        groups = sizes["gz"]
        sums = sizes["gy"] + sizes["gz"] + sizes["gx"]
        shapes = [
            (512, LANES),
            ("b", 16, 32, LANES),
            ("b", groups * SEND, 32, LANES),
            ("b", groups * SEND, 32, LANES),
            (256, LANES),
            (16, 16, LANES),
            fine,
            middle,
            low,
            (6,) + fine,
            (6,) + middle,
            (6,) + low,
            fine,
            middle,
            low,
            fine,
            middle,
            low,
            fine,
            fine,
            fine,
            middle,
            middle,
            middle,
            low,
            low,
            low,
            middle,
            middle,
            fine,
            fine,
            (8, 16, LANES),
            (12, 24, LANES),
            (12, 16, LANES),
            (2, 12, 24, LANES),
            (3, 16, LANES),
            (3, 2, 16, LANES),
            (3, 2, 16, 8, 256),
            (3, 2, 8, 8, LANES),
            (2, 2, 4, 8, LANES),
            (2, 2, 4, 8, LANES),
            (3, 8, LANES),
            (sizes["gy"], 8, LANES),
            (sizes["gz"], 8, LANES),
            (sizes["gx"], 8, LANES),
        ]
        scratch = [
            pltpu.VMEM(shape[1:], jnp.bfloat16) if shape[0] == "b" else pltpu.VMEM(shape, F32)
            for shape in shapes
        ]
        dma = pltpu.SemaphoreType.DMA
        scratch += [dma((48,)), dma((48,)), dma((groups,)), dma((groups,))]
        scratch += [dma((sums,)), dma((sums,))]
        return pl.pallas_call(
            kernel,
            out_shape=jax.ShapeDtypeStruct(coefficient.shape, F32),
            in_specs=[vmem, smem, smem, vmem],
            out_specs=vmem,
            scratch_shapes=scratch,
            compiler_params=pltpu.CompilerParams(
                collective_id=0, has_side_effects=True, vmem_limit_bytes=48 << 20
            ),
        )(old_slots, old_ids, old_owner, coefficient)

    return jax.shard_map(
        per_device,
        mesh=mesh,
        in_specs=(
            P("gx", "gy", "gz", None),
            P("gx", "gy", "gz"),
            P("gx", "gy", None),
            P("gx", "gy", "gz"),
        ),
        out_specs=P("gx", "gy", "gz"),
        check_vma=False,
    )
```

```python
import functools

import jax
import jax.numpy as jnp
from jax import lax
from jax.experimental import pallas as pl
from jax.experimental.pallas import tpu as pltpu
from jax.sharding import PartitionSpec as P

BOX = 16
NB = 8
SEND = 2
LANES = 128
MESH = pl.DeviceIdType.MESH
F32 = jnp.float32
HI = lax.Precision.HIGHEST


def iota(shape, dim):
    return lax.broadcasted_iota(jnp.int32, shape, dim)


def place(axis, step):
    count = lax.axis_size(axis)
    return {axis: lax.rem(lax.axis_index(axis) + (step + count) % count, count)}


def remote(src, dst, send, recv, axis, step):
    return pltpu.make_async_remote_copy(
        src_ref=src,
        dst_ref=dst,
        send_sem=send,
        recv_sem=recv,
        device_id=place(axis, step),
        device_id_type=MESH,
    )


def edge_scale(axis, step):
    count = lax.axis_size(axis)
    at_edge = lax.axis_index(axis) == (0 if step < 0 else count - 1)
    return jnp.where(at_edge, 0.0, 1.0).astype(F32)


class Exchange:
    def __init__(self, send, recv, base):
        self.sems = [(send.at[base + i], recv.at[base + i]) for i in range(6)]
        self.flying = []

    def pair(self, at, axis, up_src, up_dst, down_src, down_dst):
        self.flying = [
            remote(up_src, up_dst, *self.sems[at], axis, 1),
            remote(down_src, down_dst, *self.sems[at + 1], axis, -1),
        ]
        for copy in self.flying:
            copy.start()

    def land(self):
        for copy in self.flying:
            copy.wait()


class Fine(Exchange):
    def __init__(self, array, bufs, at, send, recv, base):
        self.sems = [(send.at[base + i], recv.at[base + i]) for i in range(10)]
        self.array, self.main = array, array.at[:, :, pl.ds(0, LANES)]
        names = ("edge", "packed", "z_in", "y_out", "y_in", "yp_in", "xp_in")
        for name, buf in zip(names, bufs):
            setattr(self, name, buf.at[at])
        self.all = {}

    def pair(self, at, axis, up_src, up_dst, down_src, down_dst):
        flying = [
            remote(up_src, up_dst, *self.sems[at], axis, 1),
            remote(down_src, down_dst, *self.sems[at + 1], axis, -1),
        ]
        for copy in flying:
            copy.start()
        self.all[at] = flying

    def land(self, at):
        for copy in self.all.pop(at):
            copy.wait()

    def z_start(self):
        lane, sub = iota((16, LANES), 1), iota((8, LANES), 0)
        edge = jnp.zeros((16, LANES), F32)
        for x in range(16):
            rolled = pltpu.roll(self.array[4 + x, 0:16, 0:LANES], (8 * x + 4) % LANES, 1)
            edge = jnp.where(lane // 8 == x, rolled, edge)
        self.edge[...] = edge
        self.pair(0, "gz", self.edge, self.z_in.at[0], self.edge, self.z_in.at[1])
        for x in range(8):
            near, far = self.array[4 + x, 8:16, 0:LANES], self.array[12 + x, 8:16, 0:LANES]
            self.y_out[0, x] = jnp.where(sub < 4, pltpu.roll(far, 4, 0), near)
            near, far = self.array[4 + x, 0:8, 0:LANES], self.array[12 + x, 0:8, 0:LANES]
            self.y_out[1, x] = jnp.where(sub < 4, near, pltpu.roll(far, 4, 0))
        self.pair(2, "gy", self.y_out.at[0], self.y_in.at[0], self.y_out.at[1], self.y_in.at[1])

    def z_finish(self, mask):
        self.land(0)
        lower, upper = self.z_in[0], self.z_in[1]
        if mask:
            lower, upper = lower * edge_scale("gz", -1), upper * edge_scale("gz", 1)
        self.packed[0:16, :] = jnp.where(iota((16, LANES), 1) % 8 < 4, lower, upper)

    def y_start(self):
        high, low = self.packed.at[pl.ds(8, 8)], self.packed.at[pl.ds(0, 8)]
        self.pair(4, "gy", high, self.yp_in.at[0], low, self.yp_in.at[1])

    def y_finish(self, mask):
        self.land(2)
        low = iota((8, LANES), 0) < 4
        scales = (edge_scale("gy", -1), edge_scale("gy", 1)) if mask else (1.0, 1.0)
        for x in range(8):
            lower, upper = self.y_in[0, x], self.y_in[1, x]
            if mask:
                lower, upper = lower * scales[0], upper * scales[1]
            self.array[4 + x, 16:24, 0:LANES] = jnp.where(low, upper, lower)
            self.array[12 + x, 16:24, 0:LANES] = pltpu.roll(jnp.where(low, lower, upper), 4, 0)
        main = self.main
        self.pair(
            6,
            "gx",
            main.at[pl.ds(16, 4)],
            main.at[pl.ds(0, 4)],
            main.at[pl.ds(4, 4)],
            main.at[pl.ds(20, 4)],
        )
        self.land(4)
        lower, upper = self.yp_in[0], self.yp_in[1]
        if mask:
            lower, upper = lower * scales[0], upper * scales[1]
        self.packed[16:24, :] = jnp.where(low, upper, lower)

    def x_start(self):
        self.pair(8, "gx", self.packed, self.xp_in.at[0], self.packed, self.xp_in.at[1])
        for x in range(16):
            self.array[4 + x, :, LANES:] = pltpu.roll(self.packed[...], (256 - 8 * x - 4) % 128, 1)

    def x_finish(self, mask):
        self.land(8)
        for x in range(4):
            lower = pltpu.roll(self.xp_in[0], (256 - 8 * (12 + x) - 4) % LANES, 1)
            upper = pltpu.roll(self.xp_in[1], (256 - 8 * x - 4) % LANES, 1)
            if mask:
                lower, upper = lower * edge_scale("gx", -1), upper * edge_scale("gx", 1)
            self.array[x, :, LANES:], self.array[20 + x, :, LANES:] = lower, upper
        self.land(6)
        if mask:
            self.array[0:4, :, 0:LANES] = self.array[0:4, :, 0:LANES] * edge_scale("gx", -1)
            self.array[20:24, :, 0:LANES] = self.array[20:24, :, 0:LANES] * edge_scale("gx", 1)


class Middle(Exchange):
    def __init__(self, array, z_in, *sems):
        super().__init__(*sems)
        self.array, self.z_in = array, z_in

    def z_start(self):
        own = self.array.at[pl.ds(6, 8), pl.ds(0, 8), :]
        self.pair(0, "gz", own, self.z_in.at[0], own, self.z_in.at[1])

    def z_finish(self, mask):
        self.land()
        lane = iota((8, LANES), 1)
        for x in range(8):
            lower, upper = self.z_in[0, x], self.z_in[1, x]
            if mask:
                lower, upper = lower * edge_scale("gz", -1), upper * edge_scale("gz", 1)
            halo = pltpu.roll(jnp.where(lane < 32, upper, lower), 64, 1)
            self.array[6 + x, 0:8, :] = jnp.where(lane < 64, self.array[6 + x, 0:8, :], halo)

    def y_start(self):
        rows = self.array.at[pl.ds(6, 8)]
        own = rows.at[:, pl.ds(0, 8), :]
        self.pair(2, "gy", own, rows.at[:, pl.ds(16, 8), :], own, rows.at[:, pl.ds(8, 8), :])

    def y_finish(self, mask):
        self.land()
        if mask:
            self.array[6:14, 16:24, :] = self.array[6:14, 16:24, :] * edge_scale("gy", -1)
            self.array[6:14, 8:16, :] = self.array[6:14, 8:16, :] * edge_scale("gy", 1)

    def x_start(self):
        a = self.array
        self.pair(
            4, "gx", a.at[pl.ds(8, 6)], a.at[pl.ds(0, 6)], a.at[pl.ds(6, 6)], a.at[pl.ds(14, 6)]
        )

    def x_finish(self, mask):
        self.land()
        if mask:
            self.array[0:6] = self.array[0:6] * edge_scale("gx", -1)
            self.array[14:20] = self.array[14:20] * edge_scale("gx", 1)


class Low(Exchange):
    def __init__(self, array, z_in, y_in, *sems):
        super().__init__(*sems)
        self.array, self.z_in, self.y_in = array, z_in, y_in

    def z_start(self):
        own = self.array.at[pl.ds(4, 4), pl.ds(0, 8), :]
        self.pair(0, "gz", own, self.z_in.at[0], own, self.z_in.at[1])

    def z_finish(self, mask):
        self.land()
        lane = iota((8, LANES), 1)
        for x in range(4):
            lower, upper = self.z_in[0, x], self.z_in[1, x]
            if mask:
                lower, upper = lower * edge_scale("gz", -1), upper * edge_scale("gz", 1)
            halo = jnp.where(lane < 64, pltpu.roll(upper, 32, 1), pltpu.roll(lower, 96, 1))
            self.array[4 + x, 0:8, :] = jnp.where(lane < 32, self.array[4 + x, 0:8, :], halo)

    def y_start(self):
        own = self.array.at[pl.ds(4, 4), pl.ds(0, 8), :]
        self.pair(2, "gy", own, self.y_in.at[0], own, self.y_in.at[1])

    def y_finish(self, mask):
        self.land()
        sub = iota((8, LANES), 0)
        for x in range(4):
            lower, upper = self.y_in[0, x], self.y_in[1, x]
            if mask:
                lower, upper = lower * edge_scale("gy", -1), upper * edge_scale("gy", 1)
            own = self.array[4 + x, 0:8, :]
            self.array[4 + x, 0:8, :] = jnp.where(sub < 4, own, pltpu.roll(upper, 4, 0))
            self.array[4 + x, 8:16, :] = pltpu.roll(lower, 4, 0)

    def x_start(self):
        a = self.array
        self.pair(
            4, "gx", a.at[pl.ds(4, 4)], a.at[pl.ds(0, 4)], a.at[pl.ds(4, 4)], a.at[pl.ds(8, 4)]
        )

    def x_finish(self, mask):
        self.land()
        if mask:
            self.array[0:4] = self.array[0:4] * edge_scale("gx", -1)
            self.array[8:12] = self.array[8:12] * edge_scale("gx", 1)


def in_pieces(low, high, size, piece):
    count = (high - low) // size

    def body(at, _):
        piece(low + at * size, size)
        return 0

    lax.fori_loop(0, count, body, 0)
    if low + count * size < high:
        piece(low + count * size, high - low - count * size)


def make_stencil(kappa, scaled, diagonal, inverse):
    planes, rows, lanes = kappa.shape

    def piece(x, size):
        wide = kappa[pl.ds(x - 1, size + 2)]
        here = wide[1:-1]
        around = (
            wide[:-2],
            wide[2:],
            pltpu.roll(here, 1, 1),
            pltpu.roll(here, rows - 1, 1),
            pltpu.roll(here, 1, 2),
            pltpu.roll(here, lanes - 1, 2),
        )
        faces = [0.5 * (here + other) for other in around]
        total = faces[0] + faces[1] + faces[2] + faces[3] + faces[4] + faces[5]
        inside = here > 0.0
        inv = jnp.where(inside, 1.0 / total, 0.0)
        diagonal[pl.ds(x, size)] = jnp.where(inside, total, 0.0)
        inverse[pl.ds(x, size)] = inv
        for at in range(6):
            scaled[at, pl.ds(x, size)] = faces[at] * inv

    in_pieces(1, planes - 1, 2, piece)


def around_sum(scaled, values, x, size):
    rows, lanes = scaled.shape[2:]
    wide = values[pl.ds(x - 1, size + 2)]
    here = wide[1:-1]
    face = [scaled.at[at, pl.ds(x, size)] for at in range(6)]
    total = face[0][...] * wide[:-2] + face[1][...] * wide[2:]
    total += face[2][...] * pltpu.roll(here, 1, 1)
    total += face[3][...] * pltpu.roll(here, rows - 1, 1)
    total += face[4][...] * pltpu.roll(here, 1, 2)
    total += face[5][...] * pltpu.roll(here, lanes - 1, 2)
    return here, total


def half_sweep(scaled, low, high, colour, pairs, size):
    rows, lanes = scaled.shape[2:]
    parity = (iota((rows, lanes), 0) + iota((rows, lanes), 1)) % 2

    def piece(x, count):
        for values, source in pairs:
            here, total = around_sum(scaled, values, x, count)
            if source is not None:
                total += source[pl.ds(x, count)]
            for at in range(count):
                chosen = parity == (low + at + colour) % 2
                values[x + at] = jnp.where(chosen, total[at], here[at])

    in_pieces(low, high, size, piece)


def first_red(values, source, kappa):
    planes, rows, lanes = values.shape
    parity = (iota((rows, lanes), 0) + iota((rows, lanes), 1)) % 2

    def piece(x, count):
        for at in range(count):
            kept = jnp.where(kappa[x + at] > 0.0, source[x + at], 0.0)
            source[x + at] = kept
            values[x + at] = jnp.where(parity == at % 2, kept, 0.0)

    in_pieces(0, planes, 4, piece)


def pair_matrix():
    return jnp.where(iota((LANES, LANES), 0) // 2 == iota((LANES, LANES), 1), 1.0, 0.0).astype(F32)


def coarsen(planes, shelf):
    count = planes.shape[0] // 2
    rows = planes.shape[1]
    halves = planes.reshape(count, 2, rows, LANES)
    summed = halves[:, 0] + halves[:, 1]
    shelf[0:count, 0:rows, :] = summed
    if rows == 8:
        shelf[0:count, 8:16, :] = jnp.zeros((count, 8, LANES), F32)
    even = shelf[0:count, pl.ds(0, 8, stride=2), :]
    odd = shelf[0:count, pl.ds(1, 8, stride=2), :]
    flat = (even + odd).reshape(count * 8, LANES)
    out = jnp.dot(flat, pair_matrix(), precision=HI, preferred_element_type=F32)
    return 0.125 * out.reshape(count, 8, LANES)


def refine_low(values, shelf, target):
    coarse, lane = iota((LANES, LANES), 0), iota((LANES, LANES), 1)
    wanted = jnp.where(lane < 96, lane // 2, 64 + lane // 2)
    matrix = jnp.where(coarse == wanted, 1.0, 0.0).astype(F32)
    flat = values.reshape(12 * 16, LANES)
    wide = jnp.dot(flat, matrix, precision=HI, preferred_element_type=F32).reshape(12, 16, LANES)
    for x in range(12):
        for odd in range(2):
            shelf[x, pl.ds(odd, 8, stride=2), :] = wide[x, 0:8]
            shelf[x, pl.ds(16 + odd, 4, stride=2), :] = wide[x, 12:16]
    for x in range(20):
        target[x] = shelf[(x + 2) // 2]


def refine_middle(values, narrow, shelf, target, added, kappa):
    coarse, lane = iota((LANES, 2 * LANES), 0), iota((LANES, 2 * LANES), 1)
    matrix = jnp.where(coarse == lane // 2, 1.0, 0.0).astype(F32)
    sub = iota((8, LANES), 0)
    for x in range(12):
        narrow[x, 0:8, :] = values[4 + x, 0:8, :]
        tail = jnp.where(sub < 2, values[4 + x, 8:16, :], pltpu.roll(values[4 + x, 16:24, :], 4, 0))
        narrow[x, 8:16, :] = tail
    flat = narrow[...].reshape(12 * 16, LANES)
    wide = jnp.dot(flat, matrix, precision=HI, preferred_element_type=F32).reshape(12, 16, 256)
    for x in range(12):
        for half in range(2):
            part = wide[x, :, half * LANES : (half + 1) * LANES]
            for odd in range(2):
                shelf[half, x, pl.ds(odd, 8, stride=2), :] = part[0:8]
                shelf[half, x, pl.ds(16 + odd, 4, stride=2), :] = part[8:12]
    for x in range(24):
        for half in range(2):
            lanes = slice(half * LANES, (half + 1) * LANES)
            fresh = shelf[half, x // 2]
            if added is not None:
                fresh = jnp.where(kappa[x, :, lanes] > 0.0, fresh + added[x, :, lanes], 0.0)
            target[x, :, lanes] = fresh


def pack_boxes(slots, ids, stage, boxes, outgoing):
    for piece in range(32):
        stage[piece * 16 : (piece + 1) * 16, :] = slots[
            0, 0, :, piece * LANES : (piece + 1) * LANES
        ].astype(F32)
    for slot in range(16):
        boxes[slot] = stage[pl.ds(slot, 32, stride=16), :].astype(jnp.bfloat16)
    held = [ids[0, 0, slot] for slot in range(16)]
    targets = [lax.shift_right_arithmetic(box, 3) for box in held]
    keys = [box * 16 + slot for slot, box in enumerate(held)]

    def body(group, _):
        least, most = jnp.int32(1 << 20), jnp.int32(0)
        for target, key in zip(targets, keys):
            here = target == group
            least = jnp.where(here, jnp.minimum(least, key), least)
            most = jnp.where(here, jnp.maximum(most, key), most)
        outgoing[2 * group] = boxes[jnp.bitwise_and(least, 15)]
        outgoing[2 * group + 1] = boxes[jnp.bitwise_and(most, 15)]
        return 0

    lax.fori_loop(0, outgoing.shape[0] // SEND, body, 0)


def unpack_boxes(incoming, owner, shelf, source):
    me = lax.axis_index("gz")
    owners = [owner[0, 0, me * NB + at] for at in range(NB)]
    planes = []
    for at in range(NB):
        rank = jnp.int32(0)
        for before in range(at):
            rank = jnp.where(owners[before] == owners[at], 1, rank)
        planes.append(incoming[owners[at] * SEND + rank].astype(F32))
    group = iota((32, LANES), 1) // BOX
    for row in range(8):
        merged = jnp.zeros((32, LANES), F32)
        for at in range(NB):
            rolled = pltpu.roll(planes[at], (BOX * (at - row)) % LANES, 1)
            merged = jnp.where(group == at, rolled, merged)
        shelf[row * 32 : (row + 1) * 32, :] = merged
    for x in range(16):
        for half in range(2):
            source[x, half * 8 : half * 8 + 8, :] = shelf[pl.ds(2 * x + half, 8, stride=32), :]


class AllSum:
    def __init__(self, axis, out, into, send, recv, base):
        self.axis, self.out, self.into = axis, out, into
        self.count = lax.axis_size(axis)
        self.send, self.recv, self.base = send, recv, base

    def start(self, tile):
        self.out[...] = tile
        self.flying = []
        for step in range(1, self.count):
            sems = (self.send.at[self.base + step], self.recv.at[self.base + step])
            copy = remote(self.out, self.into.at[step], *sems, self.axis, step)
            copy.start()
            self.flying.append(copy)

    def finish(self):
        for copy in self.flying:
            copy.wait()
        total = self.out[...]
        for step in range(1, self.count):
            total += self.into[step]
        return total


def kernel(
    slots_in,
    ids_in,
    owner_in,
    coefficient,
    out,
    stage,
    boxes,
    outgoing,
    incoming,
    box_shelf,
    source,
    kap0,
    kap1,
    kap2,
    sc0,
    sc1,
    sc2,
    dia0,
    dia1,
    dia2,
    inv0,
    inv1,
    inv2,
    g0,
    u0,
    w0,
    g1,
    u1,
    w1,
    f2,
    p2,
    v2,
    b1,
    c1,
    b0,
    c0,
    shelf_c,
    shelf_r1,
    narrow,
    shelf_r0,
    edge,
    packed,
    z0_in,
    y0_out,
    y0_in,
    yp0_in,
    xp0_in,
    z1_in,
    z2_in,
    y2_in,
    sum_out,
    sum_y,
    sum_z,
    sum_x,
    send,
    recv,
    box_send,
    box_recv,
    sum_send,
    sum_recv,
    slots,
    ids,
    owner,
    load_sem,
):
    loads = [
        pltpu.make_async_copy(coefficient, kap0.at[pl.ds(4, 16), pl.ds(0, 16), pl.ds(0, LANES)], load_sem.at[0]),
        pltpu.make_async_copy(slots_in, slots, load_sem.at[1]),
        pltpu.make_async_copy(ids_in, ids, load_sem.at[2]),
        pltpu.make_async_copy(owner_in, owner, load_sem.at[3]),
    ]
    for load in loads:
        load.start()
    groups = lax.axis_size("gz")
    barrier = pltpu.get_barrier_semaphore()
    partners = 0
    for axis in ("gz", "gy", "gx"):
        for step in range(1, lax.axis_size(axis)):
            pl.semaphore_signal(barrier, inc=1, device_id=place(axis, step), device_id_type=MESH)
            partners += 1

    for load in loads:
        load.wait()
    fine_bufs = (edge, packed, z0_in, y0_out, y0_in, yp0_in, xp0_in)
    pack_boxes(slots, ids, stage, boxes, outgoing)

    pl.semaphore_wait(barrier, partners)

    ex_k0 = Fine(kap0, fine_bufs, 0, send, recv, 0)
    ex_k0.z_start()

    me = lax.axis_index("gz")
    moves = []
    for step in range(1, groups):
        there = place("gz", step)["gz"]
        copy = remote(
            outgoing.at[pl.ds(SEND * there, SEND)],
            incoming.at[pl.ds(SEND * me, SEND)],
            box_send.at[step],
            box_recv.at[step],
            "gz",
            step,
        )
        copy.start()
        moves.append(copy)
    incoming[pl.ds(SEND * me, SEND)] = outgoing[pl.ds(SEND * me, SEND)]

    mid = coarsen(kap0[4:20, 0:16, 0:LANES], shelf_c)
    kap1[6:14, 0:8, :] = mid
    kap2[4:8, 0:8, :] = coarsen(mid, shelf_c)
    ex_k1 = Middle(kap1, z1_in.at[0], send, recv, 30)
    ex_k2 = Low(kap2, z2_in.at[0], y2_in.at[0], send, recv, 36)
    ex_k0.z_finish(True)
    ex_k0.y_start()
    ex_k1.z_start()
    ex_k2.z_start()
    ex_k0.y_finish(True)
    ex_k0.x_start()
    ex_k1.z_finish(True)
    ex_k1.y_start()
    ex_k2.z_finish(True)
    ex_k2.y_start()
    ex_k0.x_finish(True)
    make_stencil(kap0, sc0, dia0, inv0)
    ex_k1.y_finish(True)
    ex_k1.x_start()
    ex_k2.y_finish(True)
    ex_k2.x_start()

    for copy in moves:
        copy.wait()
    unpack_boxes(incoming, owner, box_shelf, source)

    g0[4:20, 0:16, 0:LANES] = source[...] * inv0[4:20, 0:16, 0:LANES]
    ex_g0 = Fine(g0, fine_bufs, 1, send, recv, 10)
    ex_g0.z_start()
    ex_k1.x_finish(True)
    ex_k2.x_finish(True)
    ex_g0.z_finish(False)
    ex_g0.y_start()
    make_stencil(kap1, sc1, dia1, inv1)
    ex_g0.y_finish(False)
    ex_g0.x_start()
    make_stencil(kap2, sc2, dia2, inv2)
    ex_g0.x_finish(False)
    first_red(u0, g0, kap0)
    half_sweep(sc0, 1, 23, 1, ((u0, g0),), 4)
    half_sweep(sc0, 2, 22, 0, ((u0, g0),), 4)
    half_sweep(sc0, 3, 21, 1, ((u0, g0),), 4)
    w0[4:20, 0:16, 0:LANES] = u0[4:20, 0:16, 0:LANES]

    def residual(x, count):
        here, total = around_sum(sc0, u0, x, count)
        rest = dia0[pl.ds(x, count)] * (g0[pl.ds(x, count)] + total - here)
        source[pl.ds(x - 4, count)] = rest[:, 0:16, 0:LANES]

    in_pieces(4, 20, 4, residual)

    g1[6:14, 0:8, :] = 4.0 * coarsen(source[...], shelf_c) * inv1[6:14, 0:8, :]
    ex_g1 = Middle(g1, z1_in.at[1], send, recv, 42)
    ex_w0 = Fine(w0, fine_bufs, 2, send, recv, 20)
    ex_g1.z_start()
    ex_g1.z_finish(False)
    ex_g1.y_start()
    ex_g1.y_finish(False)
    ex_g1.x_start()
    ex_w0.z_start()
    ex_g1.x_finish(False)
    first_red(u1, g1, kap1)
    half_sweep(sc1, 1, 19, 1, ((u1, g1),), 6)
    half_sweep(sc1, 2, 18, 0, ((u1, g1),), 8)
    half_sweep(sc1, 3, 17, 1, ((u1, g1),), 14)
    w1[6:14, 0:8, :] = u1[6:14, 0:8, :]

    here, total = around_sum(sc1, u1, 6, 8)
    rest = (0.25 * dia1[6:14]) * (g1[6:14] + total - here)
    f2[4:8, 0:8, :] = coarsen(rest[:, 0:8], shelf_c)
    ex_f2 = Low(f2, z2_in.at[1], y2_in.at[1], send, recv, 48)
    ex_w1 = Middle(w1, z1_in.at[2], send, recv, 54)
    ex_f2.z_start()
    ex_w1.z_start()
    ex_f2.z_finish(False)
    ex_f2.y_start()
    ex_w0.z_finish(False)
    ex_w0.y_start()
    ex_w1.z_finish(False)
    ex_w1.y_start()
    ex_f2.y_finish(False)
    ex_f2.x_start()
    ex_w0.y_finish(False)
    ex_w0.x_start()
    ex_f2.x_finish(False)
    p2[...] = jnp.where(kap2[...] > 0.0, f2[...], 0.0)

    v2[0] = jnp.zeros((16, LANES), F32)
    v2[11] = jnp.zeros((16, LANES), F32)
    here, total = around_sum(sc2, p2, 1, 10)
    v2[1:11] = (0.0625 * dia2[1:11]) * (here - total)
    own = jnp.logical_and(iota((8, LANES), 0) < 4, iota((8, LANES), 1) < 32)
    image, total = around_sum(sc2, v2, 4, 4)
    second = ((0.0625 * dia2[4:8]) * (image - total))[:, 0:8]
    image, here = image[:, 0:8], p2[4:8, 0:8, :]
    products = (
        here * here,
        here * image,
        image * image,
        second * here,
        second * image,
        second * second,
    )
    sums = [jnp.where(own, jnp.sum(product, axis=0), 0.0) for product in products]
    tile = jnp.zeros((8, LANES), F32)
    for at in range(6):
        line = jnp.sum(sums[at], axis=0, keepdims=True)
        tile = jnp.where(iota((8, LANES), 0) == at, line, tile)

    sum_gy = AllSum("gy", sum_out.at[0], sum_y, sum_send, sum_recv, 0)
    sum_gz = AllSum("gz", sum_out.at[1], sum_z, sum_send, sum_recv, lax.axis_size("gy"))
    sum_gx = AllSum(
        "gx", sum_out.at[2], sum_x, sum_send, sum_recv, lax.axis_size("gy") + groups
    )
    sum_gy.start(tile)
    ex_w1.y_finish(False)
    ex_w1.x_start()

    refine_low(p2[...], shelf_r1, b1)
    refine_low(v2[...], shelf_r1, c1)
    ex_w1.x_finish(False)
    sum_gz.start(sum_gy.finish())
    u1[...] = jnp.where(kap1[...] > 0.0, w1[...], 0.0)
    triple = ((u1, g1), (b1, None), (c1, None))
    half_sweep(sc1, 1, 19, 0, triple, 6)
    half_sweep(sc1, 2, 18, 1, triple, 8)
    half_sweep(sc1, 3, 17, 0, triple, 14)
    half_sweep(sc1, 4, 16, 1, triple, 6)

    ex_w0.x_finish(False)
    refine_middle(u1, narrow, shelf_r0, u0, w0, kap0)
    sum_gx.start(sum_gz.finish())
    refine_middle(b1, narrow, shelf_r0, b0, None, None)
    refine_middle(c1, narrow, shelf_r0, c0, None, None)
    triple = ((u0, g0), (b0, None), (c0, None))
    half_sweep(sc0, 1, 23, 0, triple, 4)
    half_sweep(sc0, 2, 22, 1, triple, 4)
    half_sweep(sc0, 3, 21, 0, triple, 4)
    half_sweep(sc0, 4, 20, 1, triple, 4)

    totals = jnp.sum(sum_gx.finish(), axis=1, keepdims=True)
    norm_rhs, along, norm_image, second_rhs, second_along, norm_second = (
        totals[at : at + 1, :] for at in range(6)
    )
    alpha = norm_rhs / along
    turned_rest = along - alpha * norm_image - alpha * second_rhs + alpha * alpha * second_along
    turned_norm = norm_image - 2.0 * alpha * second_along + alpha * alpha * norm_second
    omega = turned_rest / turned_norm
    first = jnp.broadcast_to(alpha + omega, (16, LANES))
    other = jnp.broadcast_to(alpha * omega, (16, LANES))

    def combine(x, _):
        at = (x + 4, slice(0, 16), slice(0, LANES))
        out[x] = u0[at] + first * b0[at] - other * c0[at]
        return 0

    lax.fori_loop(0, 16, combine, 0)


def solution(mesh):
    sizes = dict(mesh.shape)

    def per_device(old_slots, old_ids, old_owner, coefficient):
        vmem = pl.BlockSpec(memory_space=pltpu.VMEM)
        far = pl.BlockSpec(memory_space=pltpu.HBM)
        fine, middle, low = (24, 24, 256), (20, 24, 128), (12, 16, 128)
        groups = sizes["gz"]
        sums = sizes["gy"] + sizes["gz"] + sizes["gx"]
        shapes = [
            (512, LANES),
            ("b", 16, 32, LANES),
            ("b", groups * SEND, 32, LANES),
            ("b", groups * SEND, 32, LANES),
            (256, LANES),
            (16, 16, LANES),
            fine,
            middle,
            low,
            (6,) + fine,
            (6,) + middle,
            (6,) + low,
            fine,
            middle,
            low,
            fine,
            middle,
            low,
            fine,
            fine,
            fine,
            middle,
            middle,
            middle,
            low,
            low,
            low,
            middle,
            middle,
            fine,
            fine,
            (8, 16, LANES),
            (12, 24, LANES),
            (12, 16, LANES),
            (2, 12, 24, LANES),
            (3, 16, LANES),
            (3, 24, LANES),
            (3, 2, 16, LANES),
            (3, 2, 8, 8, LANES),
            (3, 2, 8, 8, LANES),
            (3, 2, 8, LANES),
            (3, 2, 24, LANES),
            (3, 2, 8, 8, LANES),
            (2, 2, 4, 8, LANES),
            (2, 2, 4, 8, LANES),
            (3, 8, LANES),
            (sizes["gy"], 8, LANES),
            (sizes["gz"], 8, LANES),
            (sizes["gx"], 8, LANES),
        ]
        scratch = [
            pltpu.VMEM(shape[1:], jnp.bfloat16) if shape[0] == "b" else pltpu.VMEM(shape, F32)
            for shape in shapes
        ]
        dma = pltpu.SemaphoreType.DMA
        scratch += [dma((60,)), dma((60,)), dma((groups,)), dma((groups,))]
        scratch += [dma((sums,)), dma((sums,))]
        scratch += [pltpu.VMEM(old_slots.shape, jnp.bfloat16), pltpu.SMEM(old_ids.shape, jnp.int32)]
        scratch += [pltpu.SMEM(old_owner.shape, jnp.int32), dma((4,))]
        return pl.pallas_call(
            kernel,
            out_shape=jax.ShapeDtypeStruct(coefficient.shape, F32),
            in_specs=[far] * 4,
            out_specs=vmem,
            scratch_shapes=scratch,
            compiler_params=pltpu.CompilerParams(
                collective_id=0, has_side_effects=True, vmem_limit_bytes=67_000_000
            ),
        )(old_slots, old_ids, old_owner, coefficient)

    return jax.shard_map(
        per_device,
        mesh=mesh,
        in_specs=(
            P("gx", "gy", "gz", None),
            P("gx", "gy", "gz"),
            P("gx", "gy", None),
            P("gx", "gy", "gz"),
        ),
        out_specs=P("gx", "gy", "gz"),
        check_vma=False,
    )
```

```python
import functools

import jax
import jax.numpy as jnp
from jax import lax
from jax.experimental import pallas as pl
from jax.experimental.pallas import tpu as pltpu
from jax.sharding import PartitionSpec as P

BOX = 16
NB = 8
SEND = 2
LANES = 128
MESH = pl.DeviceIdType.MESH
F32 = jnp.float32
HI = lax.Precision.HIGHEST


def iota(shape, dim):
    return lax.broadcasted_iota(jnp.int32, shape, dim)


def place(axis, step):
    count = lax.axis_size(axis)
    return {axis: lax.rem(lax.axis_index(axis) + (step + count) % count, count)}


def remote(src, dst, send, recv, axis, step):
    return pltpu.make_async_remote_copy(
        src_ref=src,
        dst_ref=dst,
        send_sem=send,
        recv_sem=recv,
        device_id=place(axis, step),
        device_id_type=MESH,
    )


def edge_scale(axis, step):
    count = lax.axis_size(axis)
    at_edge = lax.axis_index(axis) == (0 if step < 0 else count - 1)
    return jnp.where(at_edge, 0.0, 1.0).astype(F32)


NEAR = [(dx, dy, 0) for dx in (-1, 0, 1) for dy in (-1, 0, 1) if (dx, dy) != (0, 0)]
ENDS = [(dx, dy, dz) for dx in (-1, 0, 1) for dy in (-1, 0, 1) for dz in (-1, 1)]


def block(dx, dy):
    return 3 * (dx + 1) + dy + 1


def spot(dx, dy, dz):
    return {**place("gx", dx), **place("gy", dy), **place("gz", dz)}


class Direct:
    def begin(self, send, recv, base, plan):
        self.flying = []
        for at, (offset, src, dst) in enumerate(plan):
            copy = pltpu.make_async_remote_copy(
                src_ref=src,
                dst_ref=dst,
                send_sem=send.at[base + at],
                recv_sem=recv.at[base + at],
                device_id=spot(*offset),
                device_id_type=MESH,
            )
            copy.start()
            self.flying.append(copy)

    def land(self):
        for copy in self.flying:
            copy.wait()


def scales_of(mask):
    if not mask:
        return None
    return {axis: {-1: edge_scale(axis, -1), 1: edge_scale(axis, 1)} for axis in ("gx", "gy", "gz")}


def scaled_by(value, scales, dx, dy, dz):
    if scales is None:
        return value
    for axis, step in (("gx", dx), ("gy", dy), ("gz", dz)):
        if step:
            value = value * scales[axis][step]
    return value


class Middle(Direct):
    def __init__(self, array, bufs, at, send, recv, base):
        self.array, self.where = array, (send, recv, base)
        self.edge, self.main_in, self.edge_in = (buf.at[at] for buf in bufs)

    def start(self, own):
        lane = iota((8, LANES), 1)
        mirrored = pltpu.roll(own, 64, 2)
        both = own + mirrored
        edge = jnp.zeros((8, LANES), F32)
        for x in range(8):
            edge = jnp.where(lane // 16 == x, pltpu.roll(both[x], (16 * x + 8) % LANES, 1), edge)
        self.edge[...] = edge
        mine = self.main_in.at[block(0, 0)]
        for x in range(4):
            mine[x] = own[x] + mirrored[x + 4]
        plan = [
            ((dx, dy, dz), self.edge, self.edge_in.at[(1 - dz) // 2, block(-dx, -dy)])
            for dx, dy, dz in ENDS
        ]
        plan += [
            ((dx, dy, dz), mine, self.main_in.at[block(-dx, -dy)]) for dx, dy, dz in NEAR
        ]
        self.begin(*self.where, plan)

    def finish(self, mask):
        self.land()
        scales = scales_of(mask)
        lane = iota((8, LANES), 1)
        for dx, planes, first in ((-1, range(2, 8), 0), (0, range(8), 6), (1, range(6), 14)):
            for dy, row in ((0, 0), (1, 8), (-1, 16)):
                main = self.main_in.at[block(dx, dy)]
                lower = scaled_by(self.edge_in[0, block(dx, dy)], scales, dx, dy, -1)
                upper = scaled_by(self.edge_in[1, block(dx, dy)], scales, dx, dy, 1)
                for at, x in enumerate(planes):
                    own = main[x % 4] if x < 4 else pltpu.roll(main[x % 4], 64, 1)
                    own = scaled_by(own, scales, dx, dy, 0)
                    high = pltpu.roll(upper, (56 - 16 * x) % LANES, 1)
                    low = pltpu.roll(lower, (120 - 16 * x) % LANES, 1)
                    halo = jnp.where(lane < 96, high, low)
                    self.array[first + at, row : row + 8, :] = jnp.where(lane < 64, own, halo)


class Low(Direct):
    def __init__(self, array, bufs, at, send, recv, base):
        self.array, self.where = array, (send, recv, base)
        (self.tiles,) = (buf.at[at] for buf in bufs)

    def start(self, own):
        lane = iota((8, LANES), 1)
        tile = jnp.zeros((8, LANES), F32)
        for x in range(4):
            tile = jnp.where(lane // 32 == x, pltpu.roll(own[x], (32 * x) % LANES, 1), tile)
        mine = self.tiles.at[1, block(0, 0)]
        mine[...] = tile
        plan = [
            ((dx, dy, dz), mine, self.tiles.at[1 - dz, block(-dx, -dy)])
            for dx, dy, dz in ENDS + NEAR
        ]
        self.begin(*self.where, plan)

    def finish(self, mask):
        self.land()
        scales = scales_of(mask)
        lane, sub = iota((8, LANES), 1), iota((8, LANES), 0)
        for dx in (-1, 0, 1):
            firsts, seconds = [], []
            for dz in (-1, 0, 1):
                here, above, below = (
                    scaled_by(self.tiles[dz + 1, block(dx, dy)], scales, dx, dy, dz)
                    for dy in (0, 1, -1)
                )
                firsts.append(jnp.where(sub < 4, here, pltpu.roll(above, 4, 0)))
                seconds.append(jnp.where(sub < 4, 0.0, pltpu.roll(below, 4, 0)))
            for x in range(4):
                for row, parts in ((0, firsts), (8, seconds)):
                    low = pltpu.roll(parts[0], (96 - 32 * x) % LANES, 1)
                    own = pltpu.roll(parts[1], (128 - 32 * x) % LANES, 1)
                    high = pltpu.roll(parts[2], (160 - 32 * x) % LANES, 1)
                    halo = jnp.where(lane < 64, high, low)
                    self.array[4 + 4 * dx + x, row : row + 8, :] = jnp.where(lane < 32, own, halo)


class Fine:
    def __init__(self, array, bufs, at, send, recv, base):
        self.sems = [(send.at[base + i], recv.at[base + i]) for i in range(10)]
        self.array, self.main = array, array.at[:, :, pl.ds(0, LANES)]
        names = ("edge", "packed", "z_in", "y_out", "y_in", "yp_in", "xp_in")
        for name, buf in zip(names, bufs):
            setattr(self, name, buf.at[at])
        self.all = {}

    def pair(self, at, axis, up_src, up_dst, down_src, down_dst):
        flying = [
            remote(up_src, up_dst, *self.sems[at], axis, 1),
            remote(down_src, down_dst, *self.sems[at + 1], axis, -1),
        ]
        for copy in flying:
            copy.start()
        self.all[at] = flying

    def land(self, at):
        for copy in self.all.pop(at):
            copy.wait()

    def z_start(self):
        lane, sub = iota((16, LANES), 1), iota((8, LANES), 0)
        edge = jnp.zeros((16, LANES), F32)
        for x in range(16):
            rolled = pltpu.roll(self.array[4 + x, 0:16, 0:LANES], (8 * x + 4) % LANES, 1)
            edge = jnp.where(lane // 8 == x, rolled, edge)
        self.edge[...] = edge
        self.pair(0, "gz", self.edge, self.z_in.at[0], self.edge, self.z_in.at[1])
        for x in range(8):
            near, far = self.array[4 + x, 8:16, 0:LANES], self.array[12 + x, 8:16, 0:LANES]
            self.y_out[0, x] = jnp.where(sub < 4, pltpu.roll(far, 4, 0), near)
            near, far = self.array[4 + x, 0:8, 0:LANES], self.array[12 + x, 0:8, 0:LANES]
            self.y_out[1, x] = jnp.where(sub < 4, near, pltpu.roll(far, 4, 0))
        self.pair(2, "gy", self.y_out.at[0], self.y_in.at[0], self.y_out.at[1], self.y_in.at[1])

    def z_finish(self, mask):
        self.land(0)
        lower, upper = self.z_in[0], self.z_in[1]
        if mask:
            lower, upper = lower * edge_scale("gz", -1), upper * edge_scale("gz", 1)
        self.packed[0:16, :] = jnp.where(iota((16, LANES), 1) % 8 < 4, lower, upper)

    def y_start(self):
        high, low = self.packed.at[pl.ds(8, 8)], self.packed.at[pl.ds(0, 8)]
        self.pair(4, "gy", high, self.yp_in.at[0], low, self.yp_in.at[1])

    def y_finish(self, mask):
        self.land(2)
        low = iota((8, LANES), 0) < 4
        scales = (edge_scale("gy", -1), edge_scale("gy", 1)) if mask else (1.0, 1.0)
        for x in range(8):
            lower, upper = self.y_in[0, x], self.y_in[1, x]
            if mask:
                lower, upper = lower * scales[0], upper * scales[1]
            self.array[4 + x, 16:24, 0:LANES] = jnp.where(low, upper, lower)
            self.array[12 + x, 16:24, 0:LANES] = pltpu.roll(jnp.where(low, lower, upper), 4, 0)
        main = self.main
        self.pair(
            6,
            "gx",
            main.at[pl.ds(16, 4)],
            main.at[pl.ds(0, 4)],
            main.at[pl.ds(4, 4)],
            main.at[pl.ds(20, 4)],
        )
        self.land(4)
        lower, upper = self.yp_in[0], self.yp_in[1]
        if mask:
            lower, upper = lower * scales[0], upper * scales[1]
        self.packed[16:24, :] = jnp.where(low, upper, lower)

    def x_start(self):
        self.pair(8, "gx", self.packed, self.xp_in.at[0], self.packed, self.xp_in.at[1])
        for x in range(16):
            self.array[4 + x, :, LANES:] = pltpu.roll(self.packed[...], (256 - 8 * x - 4) % 128, 1)

    def x_finish(self, mask):
        self.land(8)
        for x in range(4):
            lower = pltpu.roll(self.xp_in[0], (256 - 8 * (12 + x) - 4) % LANES, 1)
            upper = pltpu.roll(self.xp_in[1], (256 - 8 * x - 4) % LANES, 1)
            if mask:
                lower, upper = lower * edge_scale("gx", -1), upper * edge_scale("gx", 1)
            self.array[x, :, LANES:], self.array[20 + x, :, LANES:] = lower, upper
        self.land(6)
        if mask:
            self.array[0:4, :, 0:LANES] = self.array[0:4, :, 0:LANES] * edge_scale("gx", -1)
            self.array[20:24, :, 0:LANES] = self.array[20:24, :, 0:LANES] * edge_scale("gx", 1)


def in_pieces(low, high, size, piece):
    count = (high - low) // size

    def body(at, _):
        piece(low + at * size, size)
        return 0

    lax.fori_loop(0, count, body, 0)
    if low + count * size < high:
        piece(low + count * size, high - low - count * size)


def make_stencil(kappa, scaled, diagonal, inverse):
    planes, rows, lanes = kappa.shape

    def piece(x, size):
        wide = kappa[pl.ds(x - 1, size + 2)]
        here = wide[1:-1]
        around = (
            wide[:-2],
            wide[2:],
            pltpu.roll(here, 1, 1),
            pltpu.roll(here, rows - 1, 1),
            pltpu.roll(here, 1, 2),
            pltpu.roll(here, lanes - 1, 2),
        )
        faces = [0.5 * (here + other) for other in around]
        total = faces[0] + faces[1] + faces[2] + faces[3] + faces[4] + faces[5]
        inside = here > 0.0
        inv = jnp.where(inside, 1.0 / total, 0.0)
        diagonal[pl.ds(x, size)] = jnp.where(inside, total, 0.0)
        inverse[pl.ds(x, size)] = inv
        for at in range(6):
            scaled[at, pl.ds(x, size)] = faces[at] * inv

    in_pieces(1, planes - 1, 2, piece)


def around_sum(scaled, values, x, size):
    rows, lanes = scaled.shape[2:]
    wide = values[pl.ds(x - 1, size + 2)]
    here = wide[1:-1]
    face = [scaled.at[at, pl.ds(x, size)] for at in range(6)]
    total = face[0][...] * wide[:-2] + face[1][...] * wide[2:]
    total += face[2][...] * pltpu.roll(here, 1, 1)
    total += face[3][...] * pltpu.roll(here, rows - 1, 1)
    total += face[4][...] * pltpu.roll(here, 1, 2)
    total += face[5][...] * pltpu.roll(here, lanes - 1, 2)
    return here, total


def half_sweep(scaled, low, high, colour, pairs, size):
    rows, lanes = scaled.shape[2:]
    parity = (iota((rows, lanes), 0) + iota((rows, lanes), 1)) % 2

    def piece(x, count):
        for values, source in pairs:
            here, total = around_sum(scaled, values, x, count)
            if source is not None:
                total += source[pl.ds(x, count)]
            for at in range(count):
                chosen = parity == (low + at + colour) % 2
                values[x + at] = jnp.where(chosen, total[at], here[at])

    in_pieces(low, high, size, piece)


def first_red(values, source, kappa):
    planes, rows, lanes = values.shape
    parity = (iota((rows, lanes), 0) + iota((rows, lanes), 1)) % 2

    def piece(x, count):
        for at in range(count):
            kept = jnp.where(kappa[x + at] > 0.0, source[x + at], 0.0)
            source[x + at] = kept
            values[x + at] = jnp.where(parity == at % 2, kept, 0.0)

    in_pieces(0, planes, 4, piece)


def pair_matrix():
    return jnp.where(iota((LANES, LANES), 0) // 2 == iota((LANES, LANES), 1), 1.0, 0.0).astype(F32)


def coarsen(planes, shelf):
    count = planes.shape[0] // 2
    rows = planes.shape[1]
    halves = planes.reshape(count, 2, rows, LANES)
    summed = halves[:, 0] + halves[:, 1]
    shelf[0:count, 0:rows, :] = summed
    if rows == 8:
        shelf[0:count, 8:16, :] = jnp.zeros((count, 8, LANES), F32)
    even = shelf[0:count, pl.ds(0, 8, stride=2), :]
    odd = shelf[0:count, pl.ds(1, 8, stride=2), :]
    flat = (even + odd).reshape(count * 8, LANES)
    out = jnp.dot(flat, pair_matrix(), precision=HI, preferred_element_type=F32)
    return 0.125 * out.reshape(count, 8, LANES)


def refine_low(values, shelf, target):
    coarse, lane = iota((LANES, LANES), 0), iota((LANES, LANES), 1)
    wanted = jnp.where(lane < 96, lane // 2, 64 + lane // 2)
    matrix = jnp.where(coarse == wanted, 1.0, 0.0).astype(F32)
    flat = values.reshape(12 * 16, LANES)
    wide = jnp.dot(flat, matrix, precision=HI, preferred_element_type=F32).reshape(12, 16, LANES)
    for x in range(12):
        for odd in range(2):
            shelf[x, pl.ds(odd, 8, stride=2), :] = wide[x, 0:8]
            shelf[x, pl.ds(16 + odd, 4, stride=2), :] = wide[x, 12:16]
    for x in range(20):
        target[x] = shelf[(x + 2) // 2]


def refine_middle(values, narrow, shelf, target, added, kappa):
    coarse, lane = iota((LANES, 2 * LANES), 0), iota((LANES, 2 * LANES), 1)
    matrix = jnp.where(coarse == lane // 2, 1.0, 0.0).astype(F32)
    sub = iota((8, LANES), 0)
    for x in range(12):
        narrow[x, 0:8, :] = values[4 + x, 0:8, :]
        tail = jnp.where(sub < 2, values[4 + x, 8:16, :], pltpu.roll(values[4 + x, 16:24, :], 4, 0))
        narrow[x, 8:16, :] = tail
    flat = narrow[...].reshape(12 * 16, LANES)
    wide = jnp.dot(flat, matrix, precision=HI, preferred_element_type=F32).reshape(12, 16, 256)
    for x in range(12):
        for half in range(2):
            part = wide[x, :, half * LANES : (half + 1) * LANES]
            for odd in range(2):
                shelf[half, x, pl.ds(odd, 8, stride=2), :] = part[0:8]
                shelf[half, x, pl.ds(16 + odd, 4, stride=2), :] = part[8:12]
    for x in range(24):
        for half in range(2):
            lanes = slice(half * LANES, (half + 1) * LANES)
            fresh = shelf[half, x // 2]
            if added is not None:
                fresh = jnp.where(kappa[x, :, lanes] > 0.0, fresh + added[x, :, lanes], 0.0)
            target[x, :, lanes] = fresh


def pack_boxes(slots, ids, stage, boxes, outgoing):
    for piece in range(32):
        stage[piece * 16 : (piece + 1) * 16, :] = slots[
            0, 0, :, piece * LANES : (piece + 1) * LANES
        ].astype(F32)
    for slot in range(16):
        boxes[slot] = stage[pl.ds(slot, 32, stride=16), :].astype(jnp.bfloat16)
    held = [ids[0, 0, slot] for slot in range(16)]
    targets = [lax.shift_right_arithmetic(box, 3) for box in held]
    keys = [box * 16 + slot for slot, box in enumerate(held)]

    def body(group, _):
        least, most = jnp.int32(1 << 20), jnp.int32(0)
        for target, key in zip(targets, keys):
            here = target == group
            least = jnp.where(here, jnp.minimum(least, key), least)
            most = jnp.where(here, jnp.maximum(most, key), most)
        outgoing[2 * group] = boxes[jnp.bitwise_and(least, 15)]
        outgoing[2 * group + 1] = boxes[jnp.bitwise_and(most, 15)]
        return 0

    lax.fori_loop(0, outgoing.shape[0] // SEND, body, 0)


def unpack_boxes(incoming, owner, shelf, source):
    me = lax.axis_index("gz")
    owners = [owner[0, 0, me * NB + at] for at in range(NB)]
    planes = []
    for at in range(NB):
        rank = jnp.int32(0)
        for before in range(at):
            rank = jnp.where(owners[before] == owners[at], 1, rank)
        planes.append(incoming[owners[at] * SEND + rank].astype(F32))
    group = iota((32, LANES), 1) // BOX
    for row in range(8):
        merged = jnp.zeros((32, LANES), F32)
        for at in range(NB):
            rolled = pltpu.roll(planes[at], (BOX * (at - row)) % LANES, 1)
            merged = jnp.where(group == at, rolled, merged)
        shelf[row * 32 : (row + 1) * 32, :] = merged
    for x in range(16):
        for half in range(2):
            source[x, half * 8 : half * 8 + 8, :] = shelf[pl.ds(2 * x + half, 8, stride=32), :]


class AllSum:
    def __init__(self, axis, out, into, send, recv, base):
        self.axis, self.out, self.into = axis, out, into
        self.count = lax.axis_size(axis)
        self.send, self.recv, self.base = send, recv, base

    def start(self, tile):
        self.out[...] = tile
        self.flying = []
        for step in range(1, self.count):
            sems = (self.send.at[self.base + step], self.recv.at[self.base + step])
            copy = remote(self.out, self.into.at[step], *sems, self.axis, step)
            copy.start()
            self.flying.append(copy)

    def finish(self):
        for copy in self.flying:
            copy.wait()
        total = self.out[...]
        for step in range(1, self.count):
            total += self.into[step]
        return total


def kernel(
    slots_in,
    ids_in,
    owner_in,
    coefficient,
    out,
    stage,
    boxes,
    outgoing,
    incoming,
    box_shelf,
    source,
    kap0,
    kap1,
    kap2,
    sc0,
    sc1,
    sc2,
    dia0,
    dia1,
    dia2,
    inv0,
    inv1,
    inv2,
    g0,
    u0,
    w0,
    g1,
    u1,
    w1,
    f2,
    p2,
    v2,
    b1,
    c1,
    b0,
    c0,
    shelf_c,
    shelf_r1,
    narrow,
    shelf_r0,
    edge,
    packed,
    z0_in,
    y0_out,
    y0_in,
    yp0_in,
    xp0_in,
    edge1,
    main1_in,
    edge1_in,
    tiles2,
    sum_out,
    sum_y,
    sum_z,
    sum_x,
    send,
    recv,
    box_send,
    box_recv,
    near_send,
    near_recv,
    sum_send,
    sum_recv,
    slots,
    ids,
    owner,
    load_sem,
):
    loads = [
        pltpu.make_async_copy(coefficient, kap0.at[pl.ds(4, 16), pl.ds(0, 16), pl.ds(0, LANES)], load_sem.at[0]),
        pltpu.make_async_copy(slots_in, slots, load_sem.at[1]),
        pltpu.make_async_copy(ids_in, ids, load_sem.at[2]),
        pltpu.make_async_copy(owner_in, owner, load_sem.at[3]),
    ]
    for load in loads:
        load.start()
    groups = lax.axis_size("gz")
    barrier = pltpu.get_barrier_semaphore()
    partners = [place(axis, step) for axis in ("gx", "gz") for step in range(2, lax.axis_size(axis) - 1)]
    partners += [place("gy", step) for step in range(2, lax.axis_size("gy") - 1)]
    partners += [spot(*offset) for offset in ENDS + NEAR]
    for partner in partners:
        pl.semaphore_signal(barrier, inc=1, device_id=partner, device_id_type=MESH)

    for load in loads:
        load.wait()
    fine_bufs = (edge, packed, z0_in, y0_out, y0_in, yp0_in, xp0_in)
    middle_bufs, low_bufs = (edge1, main1_in, edge1_in), (tiles2,)
    pack_boxes(slots, ids, stage, boxes, outgoing)
    mid = coarsen(kap0[4:20, 0:16, 0:LANES], shelf_c)
    low = coarsen(mid, shelf_c)

    pl.semaphore_wait(barrier, len(partners))

    ex_k0 = Fine(kap0, fine_bufs, 0, send, recv, 0)
    ex_k0.z_start()

    me = lax.axis_index("gz")
    moves = []
    for step in range(1, groups):
        there = place("gz", step)["gz"]
        copy = remote(
            outgoing.at[pl.ds(SEND * there, SEND)],
            incoming.at[pl.ds(SEND * me, SEND)],
            box_send.at[step],
            box_recv.at[step],
            "gz",
            step,
        )
        copy.start()
        moves.append(copy)
    incoming[pl.ds(SEND * me, SEND)] = outgoing[pl.ds(SEND * me, SEND)]

    ex_k0.z_finish(True)
    ex_k0.y_start()
    ex_k0.y_finish(True)
    ex_k0.x_start()
    ex_k1 = Middle(kap1, middle_bufs, 0, near_send, near_recv, 0)
    ex_k2 = Low(kap2, low_bufs, 0, near_send, near_recv, 26)
    ex_k1.start(mid)
    ex_k2.start(low)
    ex_k0.x_finish(True)
    make_stencil(kap0, sc0, dia0, inv0)

    for copy in moves:
        copy.wait()
    unpack_boxes(incoming, owner, box_shelf, source)

    g0[4:20, 0:16, 0:LANES] = source[...] * inv0[4:20, 0:16, 0:LANES]
    ex_g0 = Fine(g0, fine_bufs, 1, send, recv, 10)
    ex_g0.z_start()
    ex_g0.z_finish(False)
    ex_g0.y_start()
    ex_k1.finish(True)
    make_stencil(kap1, sc1, dia1, inv1)
    ex_g0.y_finish(False)
    ex_g0.x_start()
    ex_k2.finish(True)
    make_stencil(kap2, sc2, dia2, inv2)
    ex_g0.x_finish(False)
    first_red(u0, g0, kap0)
    half_sweep(sc0, 1, 23, 1, ((u0, g0),), 4)
    half_sweep(sc0, 2, 22, 0, ((u0, g0),), 4)
    half_sweep(sc0, 3, 21, 1, ((u0, g0),), 4)
    w0[4:20, 0:16, 0:LANES] = u0[4:20, 0:16, 0:LANES]

    def residual(x, count):
        here, total = around_sum(sc0, u0, x, count)
        rest = dia0[pl.ds(x, count)] * (g0[pl.ds(x, count)] + total - here)
        source[pl.ds(x - 4, count)] = rest[:, 0:16, 0:LANES]

    in_pieces(4, 20, 4, residual)

    ex_g1 = Middle(g1, middle_bufs, 1, near_send, near_recv, 52)
    ex_w0 = Fine(w0, fine_bufs, 2, send, recv, 20)
    ex_g1.start(4.0 * coarsen(source[...], shelf_c) * inv1[6:14, 0:8, :])
    ex_w0.z_start()
    ex_g1.finish(False)
    ex_w0.z_finish(False)
    ex_w0.y_start()
    first_red(u1, g1, kap1)
    half_sweep(sc1, 1, 19, 1, ((u1, g1),), 6)
    half_sweep(sc1, 2, 18, 0, ((u1, g1),), 8)
    half_sweep(sc1, 3, 17, 1, ((u1, g1),), 14)

    here, total = around_sum(sc1, u1, 6, 8)
    rest = (0.25 * dia1[6:14]) * (g1[6:14] + total - here)
    ex_f2 = Low(f2, low_bufs, 1, near_send, near_recv, 78)
    ex_w1 = Middle(w1, middle_bufs, 2, near_send, near_recv, 104)
    ex_f2.start(coarsen(rest[:, 0:8], shelf_c))
    ex_w1.start(jnp.where(iota((8, 8, LANES), 2) < 64, u1[6:14, 0:8, :], 0.0))
    ex_w0.y_finish(False)
    ex_w0.x_start()
    ex_f2.finish(False)
    p2[...] = jnp.where(kap2[...] > 0.0, f2[...], 0.0)

    v2[0] = jnp.zeros((16, LANES), F32)
    v2[11] = jnp.zeros((16, LANES), F32)
    here, total = around_sum(sc2, p2, 1, 10)
    v2[1:11] = (0.0625 * dia2[1:11]) * (here - total)
    own = jnp.logical_and(iota((8, LANES), 0) < 4, iota((8, LANES), 1) < 32)
    image, total = around_sum(sc2, v2, 4, 4)
    second = ((0.0625 * dia2[4:8]) * (image - total))[:, 0:8]
    image, here = image[:, 0:8], p2[4:8, 0:8, :]
    products = (
        here * here,
        here * image,
        image * image,
        second * here,
        second * image,
        second * second,
    )
    sums = [jnp.where(own, jnp.sum(product, axis=0), 0.0) for product in products]
    tile = jnp.zeros((8, LANES), F32)
    for at in range(6):
        line = jnp.sum(sums[at], axis=0, keepdims=True)
        tile = jnp.where(iota((8, LANES), 0) == at, line, tile)

    sum_gy = AllSum("gy", sum_out.at[0], sum_y, sum_send, sum_recv, 0)
    sum_gz = AllSum("gz", sum_out.at[1], sum_z, sum_send, sum_recv, lax.axis_size("gy"))
    sum_gx = AllSum(
        "gx", sum_out.at[2], sum_x, sum_send, sum_recv, lax.axis_size("gy") + groups
    )
    sum_gy.start(tile)

    refine_low(p2[...], shelf_r1, b1)
    refine_low(v2[...], shelf_r1, c1)
    sum_gz.start(sum_gy.finish())
    ex_w1.finish(False)
    u1[...] = jnp.where(kap1[...] > 0.0, w1[...], 0.0)
    triple = ((u1, g1), (b1, None), (c1, None))
    half_sweep(sc1, 1, 19, 0, triple, 6)
    half_sweep(sc1, 2, 18, 1, triple, 8)
    half_sweep(sc1, 3, 17, 0, triple, 14)
    half_sweep(sc1, 4, 16, 1, triple, 6)

    ex_w0.x_finish(False)
    refine_middle(u1, narrow, shelf_r0, u0, w0, kap0)
    sum_gx.start(sum_gz.finish())
    refine_middle(b1, narrow, shelf_r0, b0, None, None)
    refine_middle(c1, narrow, shelf_r0, c0, None, None)
    triple = ((u0, g0), (b0, None), (c0, None))
    half_sweep(sc0, 1, 23, 0, triple, 4)
    half_sweep(sc0, 2, 22, 1, triple, 4)
    half_sweep(sc0, 3, 21, 0, triple, 4)
    half_sweep(sc0, 4, 20, 1, triple, 4)

    totals = jnp.sum(sum_gx.finish(), axis=1, keepdims=True)
    norm_rhs, along, norm_image, second_rhs, second_along, norm_second = (
        totals[at : at + 1, :] for at in range(6)
    )
    alpha = norm_rhs / along
    turned_rest = along - alpha * norm_image - alpha * second_rhs + alpha * alpha * second_along
    turned_norm = norm_image - 2.0 * alpha * second_along + alpha * alpha * norm_second
    omega = turned_rest / turned_norm
    first = jnp.broadcast_to(alpha + omega, (16, LANES))
    other = jnp.broadcast_to(alpha * omega, (16, LANES))

    def combine(x, _):
        at = (x + 4, slice(0, 16), slice(0, LANES))
        out[x] = u0[at] + first * b0[at] - other * c0[at]
        return 0

    lax.fori_loop(0, 16, combine, 0)


def solution(mesh):
    sizes = dict(mesh.shape)

    def per_device(old_slots, old_ids, old_owner, coefficient):
        vmem = pl.BlockSpec(memory_space=pltpu.VMEM)
        far = pl.BlockSpec(memory_space=pltpu.HBM)
        fine, middle, low = (24, 24, 256), (20, 24, 128), (12, 16, 128)
        groups = sizes["gz"]
        sums = sizes["gy"] + sizes["gz"] + sizes["gx"]
        shapes = [
            (512, LANES),
            ("b", 16, 32, LANES),
            ("b", groups * SEND, 32, LANES),
            ("b", groups * SEND, 32, LANES),
            (256, LANES),
            (16, 16, LANES),
            fine,
            middle,
            low,
            (6,) + fine,
            (6,) + middle,
            (6,) + low,
            fine,
            middle,
            low,
            fine,
            middle,
            low,
            fine,
            fine,
            fine,
            middle,
            middle,
            middle,
            low,
            low,
            low,
            middle,
            middle,
            fine,
            fine,
            (8, 16, LANES),
            (12, 24, LANES),
            (12, 16, LANES),
            (2, 12, 24, LANES),
            (3, 16, LANES),
            (3, 24, LANES),
            (3, 2, 16, LANES),
            (3, 2, 8, 8, LANES),
            (3, 2, 8, 8, LANES),
            (3, 2, 8, LANES),
            (3, 2, 24, LANES),
            (3, 8, LANES),
            (3, 9, 4, 8, LANES),
            (3, 2, 9, 8, LANES),
            (2, 3, 9, 8, LANES),
            (3, 8, LANES),
            (sizes["gy"], 8, LANES),
            (sizes["gz"], 8, LANES),
            (sizes["gx"], 8, LANES),
        ]
        scratch = [
            pltpu.VMEM(shape[1:], jnp.bfloat16) if shape[0] == "b" else pltpu.VMEM(shape, F32)
            for shape in shapes
        ]
        dma = pltpu.SemaphoreType.DMA
        scratch += [dma((30,)), dma((30,)), dma((groups,)), dma((groups,)), dma((130,)), dma((130,))]
        scratch += [dma((sums,)), dma((sums,))]
        scratch += [pltpu.VMEM(old_slots.shape, jnp.bfloat16), pltpu.SMEM(old_ids.shape, jnp.int32)]
        scratch += [pltpu.SMEM(old_owner.shape, jnp.int32), dma((4,))]
        return pl.pallas_call(
            kernel,
            out_shape=jax.ShapeDtypeStruct(coefficient.shape, F32),
            in_specs=[far] * 4,
            out_specs=vmem,
            scratch_shapes=scratch,
            compiler_params=pltpu.CompilerParams(
                collective_id=0, has_side_effects=True, vmem_limit_bytes=67_000_000
            ),
        )(old_slots, old_ids, old_owner, coefficient)

    return jax.shard_map(
        per_device,
        mesh=mesh,
        in_specs=(
            P("gx", "gy", "gz", None),
            P("gx", "gy", "gz"),
            P("gx", "gy", None),
            P("gx", "gy", "gz"),
        ),
        out_specs=P("gx", "gy", "gz"),
        check_vma=False,
    )
```

```python
import functools

import jax
import jax.numpy as jnp
from jax import lax
from jax.experimental import pallas as pl
from jax.experimental.pallas import tpu as pltpu
from jax.sharding import PartitionSpec as P

BOX = 16
NB = 8
SEND = 2
RELAY = -1
LANES = 128
MESH = pl.DeviceIdType.MESH
F32 = jnp.float32
HI = lax.Precision.HIGHEST


def iota(shape, dim):
    return lax.broadcasted_iota(jnp.int32, shape, dim)


def place(axis, step):
    count = lax.axis_size(axis)
    return {axis: lax.rem(lax.axis_index(axis) + (step + count) % count, count)}


def remote(src, dst, send, recv, axis, step):
    return pltpu.make_async_remote_copy(
        src_ref=src,
        dst_ref=dst,
        send_sem=send,
        recv_sem=recv,
        device_id=place(axis, step),
        device_id_type=MESH,
    )


def edge_scale(axis, step):
    count = lax.axis_size(axis)
    at_edge = lax.axis_index(axis) == (0 if step < 0 else count - 1)
    return jnp.where(at_edge, 0.0, 1.0).astype(F32)


NEAR = [(dx, dy, 0) for dx in (-1, 0, 1) for dy in (-1, 0, 1) if (dx, dy) != (0, 0)]
ENDS = [(dx, dy, dz) for dx in (-1, 0, 1) for dy in (-1, 0, 1) for dz in (-1, 1)]


def block(dx, dy):
    return 3 * (dx + 1) + dy + 1


def spot(dx, dy, dz):
    return {**place("gx", dx), **place("gy", dy), **place("gz", dz)}


class Direct:
    def begin(self, send, recv, base, plan):
        self.flying = []
        for at, (offset, src, dst) in enumerate(plan):
            copy = pltpu.make_async_remote_copy(
                src_ref=src,
                dst_ref=dst,
                send_sem=send.at[base + at],
                recv_sem=recv.at[base + at],
                device_id=spot(*offset),
                device_id_type=MESH,
            )
            copy.start()
            self.flying.append(copy)

    def land(self):
        for copy in self.flying:
            copy.wait()


def scales_of(mask):
    if not mask:
        return None
    return {axis: {-1: edge_scale(axis, -1), 1: edge_scale(axis, 1)} for axis in ("gx", "gy", "gz")}


def scaled_by(value, scales, dx, dy, dz):
    if scales is None:
        return value
    for axis, step in (("gx", dx), ("gy", dy), ("gz", dz)):
        if step:
            value = value * scales[axis][step]
    return value


class Middle(Direct):
    def __init__(self, array, bufs, at, send, recv, base):
        self.array, self.where = array, (send, recv, base)
        self.edge, self.main_in, self.edge_in = (buf.at[at] for buf in bufs)

    def start(self, own):
        lane = iota((8, LANES), 1)
        mirrored = pltpu.roll(own, 64, 2)
        both = own + mirrored
        edge = jnp.zeros((8, LANES), F32)
        for x in range(8):
            edge = jnp.where(lane // 16 == x, pltpu.roll(both[x], (16 * x + 8) % LANES, 1), edge)
        self.edge[...] = edge
        mine = self.main_in.at[block(0, 0)]
        for x in range(4):
            mine[x] = own[x] + mirrored[x + 4]
        plan = [
            ((dx, dy, dz), self.edge, self.edge_in.at[(1 - dz) // 2, block(-dx, -dy)])
            for dx, dy, dz in ENDS
        ]
        plan += [
            ((dx, dy, dz), mine, self.main_in.at[block(-dx, -dy)]) for dx, dy, dz in NEAR
        ]
        self.begin(*self.where, plan)

    def finish(self, mask):
        self.land()
        scales = scales_of(mask)
        lane = iota((8, LANES), 1)
        for dx, planes, first in ((-1, range(2, 8), 0), (0, range(8), 6), (1, range(6), 14)):
            for dy, row in ((0, 0), (1, 8), (-1, 16)):
                main = self.main_in.at[block(dx, dy)]
                lower = scaled_by(self.edge_in[0, block(dx, dy)], scales, dx, dy, -1)
                upper = scaled_by(self.edge_in[1, block(dx, dy)], scales, dx, dy, 1)
                for at, x in enumerate(planes):
                    own = main[x % 4] if x < 4 else pltpu.roll(main[x % 4], 64, 1)
                    own = scaled_by(own, scales, dx, dy, 0)
                    high = pltpu.roll(upper, (56 - 16 * x) % LANES, 1)
                    low = pltpu.roll(lower, (120 - 16 * x) % LANES, 1)
                    halo = jnp.where(lane < 96, high, low)
                    self.array[first + at, row : row + 8, :] = jnp.where(lane < 64, own, halo)


class Low(Direct):
    def __init__(self, array, bufs, at, send, recv, base):
        self.array, self.where = array, (send, recv, base)
        (self.tiles,) = (buf.at[at] for buf in bufs)

    def start(self, own):
        lane = iota((8, LANES), 1)
        tile = jnp.zeros((8, LANES), F32)
        for x in range(4):
            tile = jnp.where(lane // 32 == x, pltpu.roll(own[x], (32 * x) % LANES, 1), tile)
        mine = self.tiles.at[1, block(0, 0)]
        mine[...] = tile
        plan = [
            ((dx, dy, dz), mine, self.tiles.at[1 - dz, block(-dx, -dy)])
            for dx, dy, dz in ENDS + NEAR
        ]
        self.begin(*self.where, plan)

    def finish(self, mask):
        self.land()
        scales = scales_of(mask)
        lane, sub = iota((8, LANES), 1), iota((8, LANES), 0)
        for dx in (-1, 0, 1):
            firsts, seconds = [], []
            for dz in (-1, 0, 1):
                here, above, below = (
                    scaled_by(self.tiles[dz + 1, block(dx, dy)], scales, dx, dy, dz)
                    for dy in (0, 1, -1)
                )
                firsts.append(jnp.where(sub < 4, here, pltpu.roll(above, 4, 0)))
                seconds.append(jnp.where(sub < 4, 0.0, pltpu.roll(below, 4, 0)))
            for x in range(4):
                for row, parts in ((0, firsts), (8, seconds)):
                    low = pltpu.roll(parts[0], (96 - 32 * x) % LANES, 1)
                    own = pltpu.roll(parts[1], (128 - 32 * x) % LANES, 1)
                    high = pltpu.roll(parts[2], (160 - 32 * x) % LANES, 1)
                    halo = jnp.where(lane < 64, high, low)
                    self.array[4 + 4 * dx + x, row : row + 8, :] = jnp.where(lane < 32, own, halo)


class Fine(Direct):
    def __init__(self, array, bufs, at, send, recv, base):
        self.array, self.where = array, (send, recv, base)
        self.edge, self.edge_in, self.y_out, self.y_in, self.corner_in = (buf.at[at] for buf in bufs)

    def start(self):
        lane, sub = iota((16, LANES), 1), iota((8, LANES), 0)
        edge = jnp.zeros((16, LANES), F32)
        for x in range(16):
            rolled = pltpu.roll(self.array[4 + x, 0:16, 0:LANES], (8 * x + 4) % LANES, 1)
            edge = jnp.where(lane // 8 == x, rolled, edge)
        self.edge[...] = edge
        for x in range(8):
            near, far = self.array[4 + x, 8:16, 0:LANES], self.array[12 + x, 8:16, 0:LANES]
            self.y_out[0, x] = jnp.where(sub < 4, pltpu.roll(far, 4, 0), near)
            near, far = self.array[4 + x, 0:8, 0:LANES], self.array[12 + x, 0:8, 0:LANES]
            self.y_out[1, x] = jnp.where(sub < 4, near, pltpu.roll(far, 4, 0))
        plan = []
        for dx, dy, dz in ENDS:
            rows = {0: pl.ds(0, 16), 1: pl.ds(8, 8), -1: pl.ds(0, 8)}[dy]
            into = self.edge_in.at[(1 - dz) // 2, block(-dx, -dy)]
            plan.append(((dx, dy, dz), self.edge.at[rows], into.at[rows]))
        inside = self.array.at[:, pl.ds(0, 16), pl.ds(0, LANES)]
        for dx, dy, dz in NEAR:
            if dy == 0:
                src = inside.at[pl.ds(16 if dx > 0 else 4, 4)]
                dst = inside.at[pl.ds(0 if dx > 0 else 20, 4)]
            elif dx == 0:
                src, dst = self.y_out.at[(1 - dy) // 2], self.y_in.at[(1 - dy) // 2]
            else:
                src = self.y_out.at[(1 - dy) // 2, pl.ds(4 if dx > 0 else 0, 4)]
                dst = self.corner_in.at[(1 - dx) // 2, (1 - dy) // 2]
            plan.append(((dx, dy, dz), src, dst))
        self.begin(*self.where, plan)

    def finish(self, mask):
        self.land()
        scales = scales_of(mask)
        low = iota((8, LANES), 0) < 4
        for x in range(8):
            lower = scaled_by(self.y_in[0, x], scales, 0, -1, 0)
            upper = scaled_by(self.y_in[1, x], scales, 0, 1, 0)
            self.array[4 + x, 16:24, 0:LANES] = jnp.where(low, upper, lower)
            self.array[12 + x, 16:24, 0:LANES] = pltpu.roll(jnp.where(low, lower, upper), 4, 0)
        for x in range(4):
            lower = scaled_by(self.corner_in[0, 0, x], scales, -1, -1, 0)
            upper = scaled_by(self.corner_in[0, 1, x], scales, -1, 1, 0)
            self.array[x, 16:24, 0:LANES] = pltpu.roll(jnp.where(low, lower, upper), 4, 0)
            lower = scaled_by(self.corner_in[1, 0, x], scales, 1, -1, 0)
            upper = scaled_by(self.corner_in[1, 1, x], scales, 1, 1, 0)
            self.array[20 + x, 16:24, 0:LANES] = jnp.where(low, upper, lower)
        if mask:
            for dx, first in ((-1, 0), (1, 20)):
                face = self.array[first : first + 4, 0:16, 0:LANES]
                self.array[first : first + 4, 0:16, 0:LANES] = scaled_by(face, scales, dx, 0, 0)
        for dx, planes, first in ((-1, range(12, 16), 0), (0, range(16), 4), (1, range(4), 20)):
            parts = []
            for dy, rows in ((0, slice(0, 16)), (1, slice(0, 8)), (-1, slice(8, 16))):
                lower = scaled_by(self.edge_in[0, block(dx, dy), rows], scales, dx, dy, -1)
                upper = scaled_by(self.edge_in[1, block(dx, dy), rows], scales, dx, dy, 1)
                parts.append(jnp.where(iota(lower.shape, 1) % 8 < 4, lower, upper))
            body, tail = parts[0], jnp.where(low, parts[1], parts[2])
            for at, x in enumerate(planes):
                shift = (2 * LANES - 8 * x - 4) % LANES
                self.array[first + at, 0:16, LANES:] = pltpu.roll(body, shift, 1)
                self.array[first + at, 16:24, LANES:] = pltpu.roll(tail, shift, 1)


def in_pieces(low, high, size, piece):
    count = (high - low) // size

    def body(at, _):
        piece(low + at * size, size)
        return 0

    lax.fori_loop(0, count, body, 0)
    if low + count * size < high:
        piece(low + count * size, high - low - count * size)


def make_stencil(kappa, scaled, diagonal, inverse):
    planes, rows, lanes = kappa.shape

    def piece(x, size):
        wide = kappa[pl.ds(x - 1, size + 2)]
        here = wide[1:-1]
        around = (
            wide[:-2],
            wide[2:],
            pltpu.roll(here, 1, 1),
            pltpu.roll(here, rows - 1, 1),
            pltpu.roll(here, 1, 2),
            pltpu.roll(here, lanes - 1, 2),
        )
        faces = [0.5 * (here + other) for other in around]
        total = faces[0] + faces[1] + faces[2] + faces[3] + faces[4] + faces[5]
        inside = here > 0.0
        inv = jnp.where(inside, 1.0 / total, 0.0)
        diagonal[pl.ds(x, size)] = jnp.where(inside, total, 0.0)
        inverse[pl.ds(x, size)] = inv
        for at in range(6):
            scaled[at, pl.ds(x, size)] = faces[at] * inv

    in_pieces(1, planes - 1, 2, piece)


def around_sum(scaled, values, x, size):
    rows, lanes = scaled.shape[2:]
    wide = values[pl.ds(x - 1, size + 2)]
    here = wide[1:-1]
    face = [scaled.at[at, pl.ds(x, size)] for at in range(6)]
    total = face[0][...] * wide[:-2] + face[1][...] * wide[2:]
    total += face[2][...] * pltpu.roll(here, 1, 1)
    total += face[3][...] * pltpu.roll(here, rows - 1, 1)
    total += face[4][...] * pltpu.roll(here, 1, 2)
    total += face[5][...] * pltpu.roll(here, lanes - 1, 2)
    return here, total


def half_sweep(scaled, low, high, colour, pairs, size):
    rows, lanes = scaled.shape[2:]
    parity = (iota((rows, lanes), 0) + iota((rows, lanes), 1)) % 2

    def piece(x, count):
        for values, source in pairs:
            here, total = around_sum(scaled, values, x, count)
            if source is not None:
                total += source[pl.ds(x, count)]
            for at in range(count):
                chosen = parity == (low + at + colour) % 2
                values[x + at] = jnp.where(chosen, total[at], here[at])

    in_pieces(low, high, size, piece)


def first_red(values, source, kappa):
    planes, rows, lanes = values.shape
    parity = (iota((rows, lanes), 0) + iota((rows, lanes), 1)) % 2

    def piece(x, count):
        for at in range(count):
            kept = jnp.where(kappa[x + at] > 0.0, source[x + at], 0.0)
            source[x + at] = kept
            values[x + at] = jnp.where(parity == at % 2, kept, 0.0)

    in_pieces(0, planes, 4, piece)


def first_red_scaled(values, source, inverse, factor):
    planes, rows, lanes = values.shape
    parity = (iota((rows, lanes), 0) + iota((rows, lanes), 1)) % 2

    def piece(x, count):
        for at in range(count):
            kept = factor * source[x + at] * inverse[x + at]
            source[x + at] = kept
            values[x + at] = jnp.where(parity == (1 + at) % 2, kept, 0.0)

    in_pieces(1, planes - 1, 6, piece)


def pair_matrix():
    return jnp.where(iota((LANES, LANES), 0) // 2 == iota((LANES, LANES), 1), 1.0, 0.0).astype(F32)


def coarsen(planes, shelf):
    count = planes.shape[0] // 2
    rows = planes.shape[1]
    halves = planes.reshape(count, 2, rows, LANES)
    summed = halves[:, 0] + halves[:, 1]
    shelf[0:count, 0:rows, :] = summed
    if rows == 8:
        shelf[0:count, 8:16, :] = jnp.zeros((count, 8, LANES), F32)
    even = shelf[0:count, pl.ds(0, 8, stride=2), :]
    odd = shelf[0:count, pl.ds(1, 8, stride=2), :]
    flat = (even + odd).reshape(count * 8, LANES)
    out = jnp.dot(flat, pair_matrix(), precision=HI, preferred_element_type=F32)
    return 0.125 * out.reshape(count, 8, LANES)


def refine_low(values, shelf, target):
    coarse, lane = iota((LANES, LANES), 0), iota((LANES, LANES), 1)
    wanted = jnp.where(lane < 96, lane // 2, 64 + lane // 2)
    matrix = jnp.where(coarse == wanted, 1.0, 0.0).astype(F32)
    flat = values.reshape(12 * 16, LANES)
    wide = jnp.dot(flat, matrix, precision=HI, preferred_element_type=F32).reshape(12, 16, LANES)
    for x in range(12):
        for odd in range(2):
            shelf[x, pl.ds(odd, 8, stride=2), :] = wide[x, 0:8]
            shelf[x, pl.ds(16 + odd, 4, stride=2), :] = wide[x, 12:16]
    for x in range(20):
        target[x] = shelf[(x + 2) // 2]


def refine_middle(values, narrow, shelf, target, added, kappa):
    coarse, lane = iota((LANES, 2 * LANES), 0), iota((LANES, 2 * LANES), 1)
    matrix = jnp.where(coarse == lane // 2, 1.0, 0.0).astype(F32)
    sub = iota((8, LANES), 0)
    for x in range(12):
        narrow[x, 0:8, :] = values[4 + x, 0:8, :]
        tail = jnp.where(sub < 2, values[4 + x, 8:16, :], pltpu.roll(values[4 + x, 16:24, :], 4, 0))
        narrow[x, 8:16, :] = tail
    flat = narrow[...].reshape(12 * 16, LANES)
    wide = jnp.dot(flat, matrix, precision=HI, preferred_element_type=F32).reshape(12, 16, 256)
    for x in range(12):
        for half in range(2):
            part = wide[x, :, half * LANES : (half + 1) * LANES]
            for odd in range(2):
                shelf[half, x, pl.ds(odd, 8, stride=2), :] = part[0:8]
                shelf[half, x, pl.ds(16 + odd, 4, stride=2), :] = part[8:12]
    for x in range(24):
        for half in range(2):
            lanes = slice(half * LANES, (half + 1) * LANES)
            fresh = shelf[half, x // 2]
            if added is not None:
                fresh = jnp.where(kappa[x, :, lanes] > 0.0, fresh + added[x, :, lanes], 0.0)
            target[x, :, lanes] = fresh


def pack_boxes(slots, ids, stage, boxes, outgoing):
    for piece in range(32):
        stage[piece * 16 : (piece + 1) * 16, :] = slots[
            0, 0, :, piece * LANES : (piece + 1) * LANES
        ].astype(F32)
    for slot in range(16):
        boxes[slot] = stage[pl.ds(slot, 32, stride=16), :].astype(jnp.bfloat16)
    held = [ids[0, 0, slot] for slot in range(16)]
    targets = [lax.shift_right_arithmetic(box, 3) for box in held]
    keys = [box * 16 + slot for slot, box in enumerate(held)]

    def body(group, _):
        least, most = jnp.int32(1 << 20), jnp.int32(0)
        for target, key in zip(targets, keys):
            here = target == group
            least = jnp.where(here, jnp.minimum(least, key), least)
            most = jnp.where(here, jnp.maximum(most, key), most)
        outgoing[2 * group] = boxes[jnp.bitwise_and(least, 15)]
        outgoing[2 * group + 1] = boxes[jnp.bitwise_and(most, 15)]
        return 0

    lax.fori_loop(0, outgoing.shape[0] // SEND, body, 0)


def unpack_boxes(incoming, owner, shelf, source):
    me = lax.axis_index("gz")
    owners = [owner[0, 0, me * NB + at] for at in range(NB)]
    planes = []
    for at in range(NB):
        rank = jnp.int32(0)
        for before in range(at):
            rank = jnp.where(owners[before] == owners[at], 1, rank)
        planes.append(incoming[owners[at] * SEND + rank].astype(F32))
    group = iota((32, LANES), 1) // BOX
    for row in range(8):
        merged = jnp.zeros((32, LANES), F32)
        for at in range(NB):
            rolled = pltpu.roll(planes[at], (BOX * (at - row)) % LANES, 1)
            merged = jnp.where(group == at, rolled, merged)
        shelf[row * 32 : (row + 1) * 32, :] = merged
    for x in range(16):
        for half in range(2):
            source[x, half * 8 : half * 8 + 8, :] = shelf[pl.ds(2 * x + half, 8, stride=32), :]


class AllSum:
    def __init__(self, axis, out, into, send, recv, base):
        self.axis, self.out, self.into = axis, out, into
        self.count = lax.axis_size(axis)
        self.send, self.recv, self.base = send, recv, base

    def start(self, tile):
        self.out[...] = tile
        self.flying = []
        for step in range(1, self.count):
            sems = (self.send.at[self.base + step], self.recv.at[self.base + step])
            copy = remote(self.out, self.into.at[step], *sems, self.axis, step)
            copy.start()
            self.flying.append(copy)

    def finish(self):
        for copy in self.flying:
            copy.wait()
        total = self.out[...]
        for step in range(1, self.count):
            total += self.into[step]
        return total


def kernel(
    slots_in,
    ids_in,
    owner_in,
    coefficient,
    out,
    stage,
    boxes,
    outgoing,
    incoming,
    box_shelf,
    source,
    kap0,
    kap1,
    kap2,
    sc0,
    sc1,
    sc2,
    dia0,
    dia1,
    dia2,
    inv0,
    inv1,
    inv2,
    g0,
    u0,
    w0,
    g1,
    u1,
    w1,
    f2,
    p2,
    v2,
    b1,
    c1,
    b0,
    c0,
    shelf_c,
    shelf_r1,
    narrow,
    shelf_r0,
    edge0,
    edge0_in,
    y0_out,
    y0_in,
    corner0_in,
    edge1,
    main1_in,
    edge1_in,
    tiles2,
    sum_out,
    sum_y,
    sum_z,
    sum_x,
    box_send,
    box_recv,
    near_send,
    near_recv,
    sum_send,
    sum_recv,
    slots,
    ids,
    owner,
    load_sem,
    passing,
    relay_sem,
):
    loads = [
        pltpu.make_async_copy(coefficient, kap0.at[pl.ds(4, 16), pl.ds(0, 16), pl.ds(0, LANES)], load_sem.at[0]),
        pltpu.make_async_copy(slots_in, slots, load_sem.at[1]),
        pltpu.make_async_copy(ids_in, ids, load_sem.at[2]),
        pltpu.make_async_copy(owner_in, owner, load_sem.at[3]),
    ]
    for load in loads:
        load.start()
    groups = lax.axis_size("gz")
    barrier = pltpu.get_barrier_semaphore()
    partners = [place(axis, step) for axis in ("gx", "gz") for step in range(2, lax.axis_size(axis) - 1)]
    partners += [place("gy", step) for step in range(2, lax.axis_size("gy") - 1)]
    partners += [spot(*offset) for offset in ENDS + NEAR]
    for partner in partners:
        pl.semaphore_signal(barrier, inc=1, device_id=partner, device_id_type=MESH)

    for load in loads:
        load.wait()
    fine_bufs = (edge0, edge0_in, y0_out, y0_in, corner0_in)
    middle_bufs, low_bufs = (edge1, main1_in, edge1_in), (tiles2,)
    pack_boxes(slots, ids, stage, boxes, outgoing)
    mid = coarsen(kap0[4:20, 0:16, 0:LANES], shelf_c)
    low = coarsen(mid, shelf_c)

    pl.semaphore_wait(barrier, len(partners))

    ex_k0 = Fine(kap0, fine_bufs, 0, near_send, near_recv, 130)
    ex_k0.start()

    me = lax.axis_index("gz")
    moves = []
    relay = None
    for step in sorted(range(1, groups), key=lambda step: -min(step, groups - step)):
        boxes_there = outgoing.at[pl.ds(SEND * place("gz", step)["gz"], SEND)]
        if RELAY and step == groups // 2:
            relay = remote(
                boxes_there, passing, relay_sem.at[0], relay_sem.at[1], "gz", RELAY * groups // 4
            )
            relay.start()
            continue
        copy = remote(
            boxes_there,
            incoming.at[pl.ds(SEND * me, SEND)],
            box_send.at[step],
            box_recv.at[step],
            "gz",
            step,
        )
        copy.start()
        moves.append(copy)
    incoming[pl.ds(SEND * me, SEND)] = outgoing[pl.ds(SEND * me, SEND)]

    ex_k0.finish(True)
    if relay is not None:
        relay.wait()
        origin = place("gz", -RELAY * groups // 4)["gz"]
        copy = remote(
            passing,
            incoming.at[pl.ds(SEND * origin, SEND)],
            box_send.at[groups // 2],
            box_recv.at[groups // 2],
            "gz",
            RELAY * groups // 4,
        )
        copy.start()
        moves.append(copy)
    ex_k1 = Middle(kap1, middle_bufs, 0, near_send, near_recv, 0)
    ex_k2 = Low(kap2, low_bufs, 0, near_send, near_recv, 26)
    ex_k1.start(mid)
    ex_k2.start(low)
    make_stencil(kap0, sc0, dia0, inv0)

    for copy in moves:
        copy.wait()
    unpack_boxes(incoming, owner, box_shelf, source)

    g0[4:20, 0:16, 0:LANES] = source[...] * inv0[4:20, 0:16, 0:LANES]
    ex_g0 = Fine(g0, fine_bufs, 1, near_send, near_recv, 156)
    ex_g0.start()
    ex_g0.finish(False)
    first_red(u0, g0, kap0)
    half_sweep(sc0, 1, 23, 1, ((u0, g0),), 4)
    half_sweep(sc0, 2, 22, 0, ((u0, g0),), 4)
    half_sweep(sc0, 3, 21, 1, ((u0, g0),), 4)
    w0[4:20, 0:16, 0:LANES] = u0[4:20, 0:16, 0:LANES]

    def residual(x, count):
        here, total = around_sum(sc0, u0, x, count)
        rest = dia0[pl.ds(x, count)] * (g0[pl.ds(x, count)] + total - here)
        source[pl.ds(x - 4, count)] = rest[:, 0:16, 0:LANES]

    in_pieces(4, 20, 4, residual)

    ex_g1 = Middle(g1, middle_bufs, 1, near_send, near_recv, 52)
    ex_w0 = Fine(w0, fine_bufs, 2, near_send, near_recv, 182)
    ex_g1.start(coarsen(source[...], shelf_c))
    ex_k1.finish(True)
    make_stencil(kap1, sc1, dia1, inv1)
    ex_k2.finish(True)
    make_stencil(kap2, sc2, dia2, inv2)
    ex_w0.start()
    ex_g1.finish(False)
    first_red_scaled(u1, g1, inv1, 4.0)
    half_sweep(sc1, 3, 17, 1, ((u1, g1),), 14)
    half_sweep(sc1, 4, 16, 0, ((u1, g1),), 6)
    half_sweep(sc1, 5, 15, 1, ((u1, g1),), 10)

    here, total = around_sum(sc1, u1, 6, 8)
    rest = (0.25 * dia1[6:14]) * (g1[6:14] + total - here)
    ex_f2 = Low(f2, low_bufs, 1, near_send, near_recv, 78)
    ex_w1 = Middle(w1, middle_bufs, 2, near_send, near_recv, 104)
    ex_f2.start(coarsen(rest[:, 0:8], shelf_c))
    ex_w1.start(jnp.where(iota((8, 8, LANES), 2) < 64, u1[6:14, 0:8, :], 0.0))
    ex_f2.finish(False)
    p2[...] = jnp.where(kap2[...] > 0.0, f2[...], 0.0)

    v2[0] = jnp.zeros((16, LANES), F32)
    v2[11] = jnp.zeros((16, LANES), F32)
    here, total = around_sum(sc2, p2, 1, 10)
    v2[1:11] = (0.0625 * dia2[1:11]) * (here - total)
    own = jnp.logical_and(iota((8, LANES), 0) < 4, iota((8, LANES), 1) < 32)
    image, total = around_sum(sc2, v2, 4, 4)
    second = ((0.0625 * dia2[4:8]) * (image - total))[:, 0:8]
    image, here = image[:, 0:8], p2[4:8, 0:8, :]
    products = (
        here * here,
        here * image,
        image * image,
        second * here,
        second * image,
        second * second,
    )
    sums = [jnp.where(own, jnp.sum(product, axis=0), 0.0) for product in products]
    tile = jnp.zeros((8, LANES), F32)
    for at in range(6):
        line = jnp.sum(sums[at], axis=0, keepdims=True)
        tile = jnp.where(iota((8, LANES), 0) == at, line, tile)

    sum_gy = AllSum("gy", sum_out.at[0], sum_y, sum_send, sum_recv, 0)
    sum_gz = AllSum("gz", sum_out.at[1], sum_z, sum_send, sum_recv, lax.axis_size("gy"))
    sum_gx = AllSum(
        "gx", sum_out.at[2], sum_x, sum_send, sum_recv, lax.axis_size("gy") + groups
    )
    sum_gy.start(tile)

    refine_low(p2[...], shelf_r1, b1)
    refine_low(v2[...], shelf_r1, c1)
    sum_gz.start(sum_gy.finish())
    ex_w1.finish(False)
    u1[...] = jnp.where(kap1[...] > 0.0, w1[...], 0.0)
    triple = ((u1, g1), (b1, None), (c1, None))
    half_sweep(sc1, 1, 19, 0, triple, 6)
    half_sweep(sc1, 2, 18, 1, triple, 8)
    half_sweep(sc1, 3, 17, 0, triple, 14)
    half_sweep(sc1, 4, 16, 1, triple, 6)

    ex_w0.finish(False)
    refine_middle(u1, narrow, shelf_r0, u0, w0, kap0)
    sum_gx.start(sum_gz.finish())
    refine_middle(b1, narrow, shelf_r0, b0, None, None)
    refine_middle(c1, narrow, shelf_r0, c0, None, None)
    triple = ((u0, g0), (b0, None), (c0, None))
    half_sweep(sc0, 1, 23, 0, triple, 4)
    half_sweep(sc0, 2, 22, 1, triple, 4)
    half_sweep(sc0, 3, 21, 0, triple, 4)
    half_sweep(sc0, 4, 20, 1, triple, 4)

    totals = jnp.sum(sum_gx.finish(), axis=1, keepdims=True)
    norm_rhs, along, norm_image, second_rhs, second_along, norm_second = (
        totals[at : at + 1, :] for at in range(6)
    )
    alpha = norm_rhs / along
    turned_rest = along - alpha * norm_image - alpha * second_rhs + alpha * alpha * second_along
    turned_norm = norm_image - 2.0 * alpha * second_along + alpha * alpha * norm_second
    omega = turned_rest / turned_norm
    first = jnp.broadcast_to(alpha + omega, (16, LANES))
    other = jnp.broadcast_to(alpha * omega, (16, LANES))

    def combine(x, _):
        at = (x + 4, slice(0, 16), slice(0, LANES))
        out[x] = u0[at] + first * b0[at] - other * c0[at]
        return 0

    lax.fori_loop(0, 16, combine, 0)


def solution(mesh):
    sizes = dict(mesh.shape)

    def per_device(old_slots, old_ids, old_owner, coefficient):
        vmem = pl.BlockSpec(memory_space=pltpu.VMEM)
        far = pl.BlockSpec(memory_space=pltpu.HBM)
        fine, middle, low = (24, 24, 256), (20, 24, 128), (12, 16, 128)
        groups = sizes["gz"]
        sums = sizes["gy"] + sizes["gz"] + sizes["gx"]
        shapes = [
            (512, LANES),
            ("b", 16, 32, LANES),
            ("b", groups * SEND, 32, LANES),
            ("b", groups * SEND, 32, LANES),
            (256, LANES),
            (16, 16, LANES),
            fine,
            middle,
            low,
            (6,) + fine,
            (6,) + middle,
            (6,) + low,
            fine,
            middle,
            low,
            fine,
            middle,
            low,
            fine,
            fine,
            fine,
            middle,
            middle,
            middle,
            low,
            low,
            low,
            middle,
            middle,
            fine,
            fine,
            (8, 16, LANES),
            (12, 24, LANES),
            (12, 16, LANES),
            (2, 12, 24, LANES),
            (3, 16, LANES),
            (3, 2, 9, 16, LANES),
            (3, 2, 8, 8, LANES),
            (3, 2, 8, 8, LANES),
            (3, 2, 2, 4, 8, LANES),
            (3, 8, LANES),
            (3, 9, 4, 8, LANES),
            (3, 2, 9, 8, LANES),
            (2, 3, 9, 8, LANES),
            (3, 8, LANES),
            (sizes["gy"], 8, LANES),
            (sizes["gz"], 8, LANES),
            (sizes["gx"], 8, LANES),
        ]
        scratch = [
            pltpu.VMEM(shape[1:], jnp.bfloat16) if shape[0] == "b" else pltpu.VMEM(shape, F32)
            for shape in shapes
        ]
        dma = pltpu.SemaphoreType.DMA
        scratch += [dma((groups,)), dma((groups,)), dma((208,)), dma((208,))]
        scratch += [dma((sums,)), dma((sums,))]
        scratch += [pltpu.VMEM(old_slots.shape, jnp.bfloat16), pltpu.SMEM(old_ids.shape, jnp.int32)]
        scratch += [pltpu.SMEM(old_owner.shape, jnp.int32), dma((4,))]
        scratch += [pltpu.VMEM((SEND, 32, LANES), jnp.bfloat16), dma((2,))]
        return pl.pallas_call(
            kernel,
            out_shape=jax.ShapeDtypeStruct(coefficient.shape, F32),
            in_specs=[far] * 4,
            out_specs=vmem,
            scratch_shapes=scratch,
            compiler_params=pltpu.CompilerParams(
                collective_id=0, has_side_effects=True, vmem_limit_bytes=67_000_000
            ),
        )(old_slots, old_ids, old_owner, coefficient)

    return jax.shard_map(
        per_device,
        mesh=mesh,
        in_specs=(
            P("gx", "gy", "gz", None),
            P("gx", "gy", "gz"),
            P("gx", "gy", None),
            P("gx", "gy", "gz"),
        ),
        out_specs=P("gx", "gy", "gz"),
        check_vma=False,
    )
```

```python
import functools

import jax
import jax.numpy as jnp
from jax import lax
from jax.experimental import pallas as pl
from jax.experimental.pallas import tpu as pltpu
from jax.sharding import PartitionSpec as P

BOX = 16
NB = 8
SEND = 2
RELAY = -1
LANES = 128
MESH = pl.DeviceIdType.MESH
F32 = jnp.float32
HI = lax.Precision.HIGHEST


def iota(shape, dim):
    return lax.broadcasted_iota(jnp.int32, shape, dim)


def place(axis, step):
    count = lax.axis_size(axis)
    return {axis: lax.rem(lax.axis_index(axis) + (step + count) % count, count)}


def remote(src, dst, send, recv, axis, step):
    return pltpu.make_async_remote_copy(
        src_ref=src,
        dst_ref=dst,
        send_sem=send,
        recv_sem=recv,
        device_id=place(axis, step),
        device_id_type=MESH,
    )


def edge_scale(axis, step):
    count = lax.axis_size(axis)
    at_edge = lax.axis_index(axis) == (0 if step < 0 else count - 1)
    return jnp.where(at_edge, 0.0, 1.0).astype(F32)


NEAR = [(dx, dy, 0) for dx in (-1, 0, 1) for dy in (-1, 0, 1) if (dx, dy) != (0, 0)]
ENDS = [(dx, dy, dz) for dx in (-1, 0, 1) for dy in (-1, 0, 1) for dz in (-1, 1)]


def block(dx, dy):
    return 3 * (dx + 1) + dy + 1


def spot(dx, dy, dz):
    return {**place("gx", dx), **place("gy", dy), **place("gz", dz)}


class Direct:
    def begin(self, send, recv, base, plan):
        self.flying = []
        for at, (offset, src, dst) in enumerate(plan):
            copy = pltpu.make_async_remote_copy(
                src_ref=src,
                dst_ref=dst,
                send_sem=send.at[base + at],
                recv_sem=recv.at[base + at],
                device_id=spot(*offset),
                device_id_type=MESH,
            )
            copy.start()
            self.flying.append(copy)

    def land(self):
        for copy in self.flying:
            copy.wait()


def scales_of(mask):
    if not mask:
        return None
    return {axis: {-1: edge_scale(axis, -1), 1: edge_scale(axis, 1)} for axis in ("gx", "gy", "gz")}


def scaled_by(value, scales, dx, dy, dz):
    if scales is None:
        return value
    for axis, step in (("gx", dx), ("gy", dy), ("gz", dz)):
        if step:
            value = value * scales[axis][step]
    return value


class Middle(Direct):
    def __init__(self, array, bufs, at, send, recv, base):
        self.array, self.where = array, (send, recv, base)
        self.edge, self.main_in, self.edge_in = (buf.at[at] for buf in bufs)

    def start(self, own):
        lane = iota((8, LANES), 1)
        mirrored = pltpu.roll(own, 64, 2)
        both = own + mirrored
        edge = jnp.zeros((8, LANES), F32)
        for x in range(8):
            edge = jnp.where(lane // 16 == x, pltpu.roll(both[x], (16 * x + 8) % LANES, 1), edge)
        self.edge[...] = edge
        mine = self.main_in.at[block(0, 0)]
        for x in range(4):
            mine[x] = own[x] + mirrored[x + 4]
        plan = [
            ((dx, dy, dz), self.edge, self.edge_in.at[(1 - dz) // 2, block(-dx, -dy)])
            for dx, dy, dz in ENDS
        ]
        plan += [
            ((dx, dy, dz), mine, self.main_in.at[block(-dx, -dy)]) for dx, dy, dz in NEAR
        ]
        self.begin(*self.where, plan)

    def finish(self, mask):
        self.land()
        scales = scales_of(mask)
        lane = iota((8, LANES), 1)
        for dx, planes, first in ((-1, range(2, 8), 0), (0, range(8), 6), (1, range(6), 14)):
            for dy, row in ((0, 0), (1, 8), (-1, 16)):
                main = self.main_in.at[block(dx, dy)]
                lower = scaled_by(self.edge_in[0, block(dx, dy)], scales, dx, dy, -1)
                upper = scaled_by(self.edge_in[1, block(dx, dy)], scales, dx, dy, 1)
                for at, x in enumerate(planes):
                    own = main[x % 4] if x < 4 else pltpu.roll(main[x % 4], 64, 1)
                    own = scaled_by(own, scales, dx, dy, 0)
                    high = pltpu.roll(upper, (56 - 16 * x) % LANES, 1)
                    low = pltpu.roll(lower, (120 - 16 * x) % LANES, 1)
                    halo = jnp.where(lane < 96, high, low)
                    self.array[first + at, row : row + 8, :] = jnp.where(lane < 64, own, halo)


class Low(Direct):
    def __init__(self, array, bufs, at, send, recv, base):
        self.array, self.where = array, (send, recv, base)
        (self.tiles,) = (buf.at[at] for buf in bufs)

    def start(self, own):
        lane = iota((8, LANES), 1)
        tile = jnp.zeros((8, LANES), F32)
        for x in range(4):
            tile = jnp.where(lane // 32 == x, pltpu.roll(own[x], (32 * x) % LANES, 1), tile)
        mine = self.tiles.at[1, block(0, 0)]
        mine[...] = tile
        plan = [
            ((dx, dy, dz), mine, self.tiles.at[1 - dz, block(-dx, -dy)])
            for dx, dy, dz in ENDS + NEAR
        ]
        self.begin(*self.where, plan)

    def finish(self, mask):
        self.land()
        scales = scales_of(mask)
        lane, sub = iota((8, LANES), 1), iota((8, LANES), 0)
        for dx in (-1, 0, 1):
            firsts, seconds = [], []
            for dz in (-1, 0, 1):
                here, above, below = (
                    scaled_by(self.tiles[dz + 1, block(dx, dy)], scales, dx, dy, dz)
                    for dy in (0, 1, -1)
                )
                firsts.append(jnp.where(sub < 4, here, pltpu.roll(above, 4, 0)))
                seconds.append(jnp.where(sub < 4, 0.0, pltpu.roll(below, 4, 0)))
            for x in range(4):
                for row, parts in ((0, firsts), (8, seconds)):
                    low = pltpu.roll(parts[0], (96 - 32 * x) % LANES, 1)
                    own = pltpu.roll(parts[1], (128 - 32 * x) % LANES, 1)
                    high = pltpu.roll(parts[2], (160 - 32 * x) % LANES, 1)
                    halo = jnp.where(lane < 64, high, low)
                    self.array[4 + 4 * dx + x, row : row + 8, :] = jnp.where(lane < 32, own, halo)


class Fine(Direct):
    def __init__(self, array, bufs, at, send, recv, base):
        self.array, self.where = array, (send, recv, base)
        self.edge, self.edge_in, self.y_out, self.y_in, self.corner_in = (buf.at[at] for buf in bufs)

    def start(self):
        lane, sub = iota((16, LANES), 1), iota((8, LANES), 0)
        edge = jnp.zeros((16, LANES), F32)
        for x in range(16):
            rolled = pltpu.roll(self.array[4 + x, 0:16, 0:LANES], (8 * x + 4) % LANES, 1)
            edge = jnp.where(lane // 8 == x, rolled, edge)
        self.edge[...] = edge
        for x in range(8):
            near, far = self.array[4 + x, 8:16, 0:LANES], self.array[12 + x, 8:16, 0:LANES]
            self.y_out[0, x] = jnp.where(sub < 4, pltpu.roll(far, 4, 0), near)
            near, far = self.array[4 + x, 0:8, 0:LANES], self.array[12 + x, 0:8, 0:LANES]
            self.y_out[1, x] = jnp.where(sub < 4, near, pltpu.roll(far, 4, 0))
        plan = []
        for dx, dy, dz in ENDS:
            rows = {0: pl.ds(0, 16), 1: pl.ds(8, 8), -1: pl.ds(0, 8)}[dy]
            into = self.edge_in.at[(1 - dz) // 2, block(-dx, -dy)]
            plan.append(((dx, dy, dz), self.edge.at[rows], into.at[rows]))
        inside = self.array.at[:, pl.ds(0, 16), pl.ds(0, LANES)]
        for dx, dy, dz in NEAR:
            if dy == 0:
                src = inside.at[pl.ds(16 if dx > 0 else 4, 4)]
                dst = inside.at[pl.ds(0 if dx > 0 else 20, 4)]
            elif dx == 0:
                src, dst = self.y_out.at[(1 - dy) // 2], self.y_in.at[(1 - dy) // 2]
            else:
                src = self.y_out.at[(1 - dy) // 2, pl.ds(4 if dx > 0 else 0, 4)]
                dst = self.corner_in.at[(1 - dx) // 2, (1 - dy) // 2]
            plan.append(((dx, dy, dz), src, dst))
        self.begin(*self.where, plan)

    def finish(self, mask):
        self.land()
        scales = scales_of(mask)
        low = iota((8, LANES), 0) < 4
        for x in range(8):
            lower = scaled_by(self.y_in[0, x], scales, 0, -1, 0)
            upper = scaled_by(self.y_in[1, x], scales, 0, 1, 0)
            self.array[4 + x, 16:24, 0:LANES] = jnp.where(low, upper, lower)
            self.array[12 + x, 16:24, 0:LANES] = pltpu.roll(jnp.where(low, lower, upper), 4, 0)
        for x in range(4):
            lower = scaled_by(self.corner_in[0, 0, x], scales, -1, -1, 0)
            upper = scaled_by(self.corner_in[0, 1, x], scales, -1, 1, 0)
            self.array[x, 16:24, 0:LANES] = pltpu.roll(jnp.where(low, lower, upper), 4, 0)
            lower = scaled_by(self.corner_in[1, 0, x], scales, 1, -1, 0)
            upper = scaled_by(self.corner_in[1, 1, x], scales, 1, 1, 0)
            self.array[20 + x, 16:24, 0:LANES] = jnp.where(low, upper, lower)
        if mask:
            for dx, first in ((-1, 0), (1, 20)):
                face = self.array[first : first + 4, 0:16, 0:LANES]
                self.array[first : first + 4, 0:16, 0:LANES] = scaled_by(face, scales, dx, 0, 0)
        for dx, planes, first in ((-1, range(12, 16), 0), (0, range(16), 4), (1, range(4), 20)):
            parts = []
            for dy, rows in ((0, slice(0, 16)), (1, slice(0, 8)), (-1, slice(8, 16))):
                lower = scaled_by(self.edge_in[0, block(dx, dy), rows], scales, dx, dy, -1)
                upper = scaled_by(self.edge_in[1, block(dx, dy), rows], scales, dx, dy, 1)
                parts.append(jnp.where(iota(lower.shape, 1) % 8 < 4, lower, upper))
            body, tail = parts[0], jnp.where(low, parts[1], parts[2])
            for at, x in enumerate(planes):
                shift = (2 * LANES - 8 * x - 4) % LANES
                self.array[first + at, 0:16, LANES:] = pltpu.roll(body, shift, 1)
                self.array[first + at, 16:24, LANES:] = pltpu.roll(tail, shift, 1)


def in_pieces(low, high, size, piece):
    count = (high - low) // size

    def body(at, _):
        piece(low + at * size, size)
        return 0

    lax.fori_loop(0, count, body, 0)
    if low + count * size < high:
        piece(low + count * size, high - low - count * size)


def make_stencil(kappa, scaled, diagonal, inverse):
    planes, rows, lanes = kappa.shape

    def piece(x, size):
        wide = kappa[pl.ds(x - 1, size + 2)]
        here = wide[1:-1]
        around = (
            wide[:-2],
            wide[2:],
            pltpu.roll(here, 1, 1),
            pltpu.roll(here, rows - 1, 1),
            pltpu.roll(here, 1, 2),
            pltpu.roll(here, lanes - 1, 2),
        )
        faces = [0.5 * (here + other) for other in around]
        total = faces[0] + faces[1] + faces[2] + faces[3] + faces[4] + faces[5]
        inside = here > 0.0
        inv = jnp.where(inside, 1.0 / total, 0.0)
        diagonal[pl.ds(x, size)] = jnp.where(inside, total, 0.0)
        inverse[pl.ds(x, size)] = inv
        for at in range(6):
            scaled[at, pl.ds(x, size)] = faces[at] * inv

    in_pieces(1, planes - 1, 2, piece)


def around_sum(scaled, values, x, size):
    rows, lanes = scaled.shape[2:]
    wide = values[pl.ds(x - 1, size + 2)]
    here = wide[1:-1]
    face = [scaled.at[at, pl.ds(x, size)] for at in range(6)]
    total = face[0][...] * wide[:-2] + face[1][...] * wide[2:]
    total += face[2][...] * pltpu.roll(here, 1, 1)
    total += face[3][...] * pltpu.roll(here, rows - 1, 1)
    total += face[4][...] * pltpu.roll(here, 1, 2)
    total += face[5][...] * pltpu.roll(here, lanes - 1, 2)
    return here, total


def half_sweep(scaled, low, high, colour, pairs, size):
    rows, lanes = scaled.shape[2:]
    parity = (iota((rows, lanes), 0) + iota((rows, lanes), 1)) % 2

    def piece(x, count):
        for values, source in pairs:
            here, total = around_sum(scaled, values, x, count)
            if source is not None:
                total += source[pl.ds(x, count)]
            for at in range(count):
                chosen = parity == (low + at + colour) % 2
                values[x + at] = jnp.where(chosen, total[at], here[at])

    in_pieces(low, high, size, piece)


def first_red(values, source, kappa):
    planes, rows, lanes = values.shape
    parity = (iota((rows, lanes), 0) + iota((rows, lanes), 1)) % 2

    def piece(x, count):
        for at in range(count):
            kept = jnp.where(kappa[x + at] > 0.0, source[x + at], 0.0)
            source[x + at] = kept
            values[x + at] = jnp.where(parity == at % 2, kept, 0.0)

    in_pieces(0, planes, 4, piece)


def first_red_scaled(values, source, inverse, factor):
    planes, rows, lanes = values.shape
    parity = (iota((rows, lanes), 0) + iota((rows, lanes), 1)) % 2

    def piece(x, count):
        for at in range(count):
            kept = factor * source[x + at] * inverse[x + at]
            source[x + at] = kept
            values[x + at] = jnp.where(parity == (1 + at) % 2, kept, 0.0)

    in_pieces(1, planes - 1, 6, piece)


def pair_matrix():
    return jnp.where(iota((LANES, LANES), 0) // 2 == iota((LANES, LANES), 1), 1.0, 0.0).astype(F32)


def coarsen(planes, shelf):
    count = planes.shape[0] // 2
    rows = planes.shape[1]
    halves = planes.reshape(count, 2, rows, LANES)
    summed = halves[:, 0] + halves[:, 1]
    shelf[0:count, 0:rows, :] = summed
    if rows == 8:
        shelf[0:count, 8:16, :] = jnp.zeros((count, 8, LANES), F32)
    even = shelf[0:count, pl.ds(0, 8, stride=2), :]
    odd = shelf[0:count, pl.ds(1, 8, stride=2), :]
    flat = (even + odd).reshape(count * 8, LANES)
    out = jnp.dot(flat, pair_matrix(), precision=HI, preferred_element_type=F32)
    return 0.125 * out.reshape(count, 8, LANES)


def refine_low(values, shelf, target):
    coarse, lane = iota((LANES, LANES), 0), iota((LANES, LANES), 1)
    wanted = jnp.where(lane < 96, lane // 2, 64 + lane // 2)
    matrix = jnp.where(coarse == wanted, 1.0, 0.0).astype(F32)
    flat = values.reshape(12 * 16, LANES)
    wide = jnp.dot(flat, matrix, precision=HI, preferred_element_type=F32).reshape(12, 16, LANES)
    for x in range(12):
        for odd in range(2):
            shelf[x, pl.ds(odd, 8, stride=2), :] = wide[x, 0:8]
            shelf[x, pl.ds(16 + odd, 4, stride=2), :] = wide[x, 12:16]
    for x in range(20):
        target[x] = shelf[(x + 2) // 2]


def refine_middle(values, narrow, shelf, target, added, kappa):
    coarse, lane = iota((LANES, 2 * LANES), 0), iota((LANES, 2 * LANES), 1)
    matrix = jnp.where(coarse == lane // 2, 1.0, 0.0).astype(F32)
    sub = iota((8, LANES), 0)
    for x in range(12):
        narrow[x, 0:8, :] = values[4 + x, 0:8, :]
        tail = jnp.where(sub < 2, values[4 + x, 8:16, :], pltpu.roll(values[4 + x, 16:24, :], 4, 0))
        narrow[x, 8:16, :] = tail
    flat = narrow[...].reshape(12 * 16, LANES)
    wide = jnp.dot(flat, matrix, precision=HI, preferred_element_type=F32).reshape(12, 16, 256)
    for x in range(12):
        for half in range(2):
            part = wide[x, :, half * LANES : (half + 1) * LANES]
            for odd in range(2):
                shelf[half, x, pl.ds(odd, 8, stride=2), :] = part[0:8]
                shelf[half, x, pl.ds(16 + odd, 4, stride=2), :] = part[8:12]
    for x in range(24):
        for half in range(2):
            lanes = slice(half * LANES, (half + 1) * LANES)
            fresh = shelf[half, x // 2]
            if added is not None:
                fresh = jnp.where(kappa[x, :, lanes] > 0.0, fresh + added[x, :, lanes], 0.0)
            target[x, :, lanes] = fresh


def pack_boxes(slots, ids, stage, boxes, outgoing):
    for piece in range(32):
        stage[piece * 16 : (piece + 1) * 16, :] = slots[
            0, 0, :, piece * LANES : (piece + 1) * LANES
        ].astype(F32)
    for slot in range(16):
        boxes[slot] = stage[pl.ds(slot, 32, stride=16), :].astype(jnp.bfloat16)
    held = [ids[0, 0, slot] for slot in range(16)]
    targets = [lax.shift_right_arithmetic(box, 3) for box in held]
    keys = [box * 16 + slot for slot, box in enumerate(held)]

    def body(group, _):
        least, most = jnp.int32(1 << 20), jnp.int32(0)
        for target, key in zip(targets, keys):
            here = target == group
            least = jnp.where(here, jnp.minimum(least, key), least)
            most = jnp.where(here, jnp.maximum(most, key), most)
        outgoing[2 * group] = boxes[jnp.bitwise_and(least, 15)]
        outgoing[2 * group + 1] = boxes[jnp.bitwise_and(most, 15)]
        return 0

    lax.fori_loop(0, outgoing.shape[0] // SEND, body, 0)


def unpack_boxes(incoming, owner, shelf, source):
    me = lax.axis_index("gz")
    owners = [owner[0, 0, me * NB + at] for at in range(NB)]
    planes = []
    for at in range(NB):
        rank = jnp.int32(0)
        for before in range(at):
            rank = jnp.where(owners[before] == owners[at], 1, rank)
        planes.append(incoming[owners[at] * SEND + rank].astype(F32))
    group = iota((32, LANES), 1) // BOX
    for row in range(8):
        merged = jnp.zeros((32, LANES), F32)
        for at in range(NB):
            rolled = pltpu.roll(planes[at], (BOX * (at - row)) % LANES, 1)
            merged = jnp.where(group == at, rolled, merged)
        shelf[row * 32 : (row + 1) * 32, :] = merged
    for x in range(16):
        for half in range(2):
            source[x, half * 8 : half * 8 + 8, :] = shelf[pl.ds(2 * x + half, 8, stride=32), :]


class AllSum:
    def __init__(self, axis, out, into, send, recv, base):
        self.axis, self.out, self.into = axis, out, into
        self.count = lax.axis_size(axis)
        self.send, self.recv, self.base = send, recv, base

    def start(self, tile):
        self.out[...] = tile
        self.flying = []
        for step in range(1, self.count):
            sems = (self.send.at[self.base + step], self.recv.at[self.base + step])
            copy = remote(self.out, self.into.at[step], *sems, self.axis, step)
            copy.start()
            self.flying.append(copy)

    def finish(self):
        for copy in self.flying:
            copy.wait()
        total = self.out[...]
        for step in range(1, self.count):
            total += self.into[step]
        return total


def kernel(
    slots_in,
    ids_in,
    owner_in,
    coefficient,
    out,
    stage,
    boxes,
    outgoing,
    incoming,
    box_shelf,
    source,
    kap0,
    kap1,
    kap2,
    sc0,
    sc1,
    sc2,
    dia0,
    dia1,
    dia2,
    inv0,
    inv1,
    inv2,
    g0,
    u0,
    w0,
    g1,
    u1,
    w1,
    f2,
    p2,
    v2,
    b1,
    c1,
    b0,
    c0,
    shelf_c,
    shelf_r1,
    narrow,
    shelf_r0,
    edge0,
    edge0_in,
    y0_out,
    y0_in,
    corner0_in,
    edge1,
    main1_in,
    edge1_in,
    tiles2,
    sum_out,
    sum_y,
    sum_z,
    sum_x,
    box_send,
    box_recv,
    near_send,
    near_recv,
    sum_send,
    sum_recv,
    slots,
    ids,
    owner,
    load_sem,
    passing,
    relay_sem,
):
    loads = [
        pltpu.make_async_copy(coefficient, kap0.at[pl.ds(4, 16), pl.ds(0, 16), pl.ds(0, LANES)], load_sem.at[0]),
        pltpu.make_async_copy(slots_in, slots, load_sem.at[1]),
        pltpu.make_async_copy(ids_in, ids, load_sem.at[2]),
        pltpu.make_async_copy(owner_in, owner, load_sem.at[3]),
    ]
    for load in loads:
        load.start()
    groups = lax.axis_size("gz")
    barrier = pltpu.get_barrier_semaphore()
    partners = [place(axis, step) for axis in ("gx", "gz") for step in range(2, lax.axis_size(axis) - 1)]
    partners += [place("gy", step) for step in range(2, lax.axis_size("gy") - 1)]
    partners += [spot(*offset) for offset in ENDS + NEAR]
    for partner in partners:
        pl.semaphore_signal(barrier, inc=1, device_id=partner, device_id_type=MESH)

    for load in loads:
        load.wait()
    fine_bufs = (edge0, edge0_in, y0_out, y0_in, corner0_in)
    middle_bufs, low_bufs = (edge1, main1_in, edge1_in), (tiles2,)
    pack_boxes(slots, ids, stage, boxes, outgoing)
    mid = coarsen(kap0[4:20, 0:16, 0:LANES], shelf_c)
    low = coarsen(mid, shelf_c)

    pl.semaphore_wait(barrier, len(partners))

    ex_k0 = Fine(kap0, fine_bufs, 0, near_send, near_recv, 130)
    ex_k0.start()

    me = lax.axis_index("gz")
    moves = []
    relay = None
    for step in sorted(range(1, groups), key=lambda step: -min(step, groups - step)):
        boxes_there = outgoing.at[pl.ds(SEND * place("gz", step)["gz"], SEND)]
        if RELAY and step == groups // 2:
            relay = remote(
                boxes_there, passing, relay_sem.at[0], relay_sem.at[1], "gz", RELAY * groups // 4
            )
            relay.start()
            continue
        copy = remote(
            boxes_there,
            incoming.at[pl.ds(SEND * me, SEND)],
            box_send.at[step],
            box_recv.at[step],
            "gz",
            step,
        )
        copy.start()
        moves.append(copy)
    incoming[pl.ds(SEND * me, SEND)] = outgoing[pl.ds(SEND * me, SEND)]

    ex_k0.finish(True)
    if relay is not None:
        relay.wait()
        origin = place("gz", -RELAY * groups // 4)["gz"]
        copy = remote(
            passing,
            incoming.at[pl.ds(SEND * origin, SEND)],
            box_send.at[groups // 2],
            box_recv.at[groups // 2],
            "gz",
            RELAY * groups // 4,
        )
        copy.start()
        moves.append(copy)
    ex_k1 = Middle(kap1, middle_bufs, 0, near_send, near_recv, 0)
    ex_k2 = Low(kap2, low_bufs, 0, near_send, near_recv, 26)
    ex_k1.start(mid)
    ex_k2.start(low)
    make_stencil(kap0, sc0, dia0, inv0)

    for copy in moves:
        copy.wait()
    unpack_boxes(incoming, owner, box_shelf, source)

    g0[4:20, 0:16, 0:LANES] = source[...] * inv0[4:20, 0:16, 0:LANES]
    ex_g0 = Fine(g0, fine_bufs, 1, near_send, near_recv, 156)
    ex_g0.start()
    ex_g0.finish(False)
    first_red(u0, g0, kap0)
    half_sweep(sc0, 1, 23, 1, ((u0, g0),), 6)
    half_sweep(sc0, 2, 22, 0, ((u0, g0),), 6)
    half_sweep(sc0, 3, 21, 1, ((u0, g0),), 6)
    w0[4:20, 0:16, 0:LANES] = u0[4:20, 0:16, 0:LANES]

    def residual(x, count):
        here, total = around_sum(sc0, u0, x, count)
        rest = dia0[pl.ds(x, count)] * (g0[pl.ds(x, count)] + total - here)
        source[pl.ds(x - 4, count)] = rest[:, 0:16, 0:LANES]

    in_pieces(4, 20, 8, residual)

    ex_g1 = Middle(g1, middle_bufs, 1, near_send, near_recv, 52)
    ex_w0 = Fine(w0, fine_bufs, 2, near_send, near_recv, 182)
    ex_g1.start(coarsen(source[...], shelf_c))
    ex_k1.finish(True)
    make_stencil(kap1, sc1, dia1, inv1)
    ex_k2.finish(True)
    make_stencil(kap2, sc2, dia2, inv2)
    ex_g1.finish(False)
    first_red_scaled(u1, g1, inv1, 4.0)
    half_sweep(sc1, 3, 17, 1, ((u1, g1),), 14)
    half_sweep(sc1, 4, 16, 0, ((u1, g1),), 6)
    half_sweep(sc1, 5, 15, 1, ((u1, g1),), 10)

    here, total = around_sum(sc1, u1, 6, 8)
    rest = (0.25 * dia1[6:14]) * (g1[6:14] + total - here)
    ex_f2 = Low(f2, low_bufs, 1, near_send, near_recv, 78)
    ex_w1 = Middle(w1, middle_bufs, 2, near_send, near_recv, 104)
    ex_f2.start(coarsen(rest[:, 0:8], shelf_c))
    ex_w1.start(jnp.where(iota((8, 8, LANES), 2) < 64, u1[6:14, 0:8, :], 0.0))
    ex_w0.start()
    ex_f2.finish(False)
    p2[...] = jnp.where(kap2[...] > 0.0, f2[...], 0.0)

    v2[0] = jnp.zeros((16, LANES), F32)
    v2[11] = jnp.zeros((16, LANES), F32)
    here, total = around_sum(sc2, p2, 1, 10)
    v2[1:11] = (0.0625 * dia2[1:11]) * (here - total)
    own = jnp.logical_and(iota((8, LANES), 0) < 4, iota((8, LANES), 1) < 32)
    image, total = around_sum(sc2, v2, 4, 4)
    second = ((0.0625 * dia2[4:8]) * (image - total))[:, 0:8]
    image, here = image[:, 0:8], p2[4:8, 0:8, :]
    products = (
        here * here,
        here * image,
        image * image,
        second * here,
        second * image,
        second * second,
    )
    sums = [jnp.where(own, jnp.sum(product, axis=0), 0.0) for product in products]
    tile = jnp.zeros((8, LANES), F32)
    for at in range(6):
        line = jnp.sum(sums[at], axis=0, keepdims=True)
        tile = jnp.where(iota((8, LANES), 0) == at, line, tile)

    sum_gy = AllSum("gy", sum_out.at[0], sum_y, sum_send, sum_recv, 0)
    sum_gz = AllSum("gz", sum_out.at[1], sum_z, sum_send, sum_recv, lax.axis_size("gy"))
    sum_gx = AllSum(
        "gx", sum_out.at[2], sum_x, sum_send, sum_recv, lax.axis_size("gy") + groups
    )
    sum_gy.start(tile)

    refine_low(p2[...], shelf_r1, b1)
    refine_low(v2[...], shelf_r1, c1)
    sum_gz.start(sum_gy.finish())
    ex_w1.finish(False)
    u1[...] = jnp.where(kap1[...] > 0.0, w1[...], 0.0)
    triple = ((u1, g1), (b1, None), (c1, None))
    half_sweep(sc1, 1, 19, 0, triple, 6)
    half_sweep(sc1, 2, 18, 1, triple, 8)
    half_sweep(sc1, 3, 17, 0, triple, 14)
    half_sweep(sc1, 4, 16, 1, triple, 6)

    ex_w0.finish(False)
    refine_middle(u1, narrow, shelf_r0, u0, w0, kap0)
    sum_gx.start(sum_gz.finish())
    refine_middle(b1, narrow, shelf_r0, b0, None, None)
    refine_middle(c1, narrow, shelf_r0, c0, None, None)
    triple = ((u0, g0), (b0, None), (c0, None))
    half_sweep(sc0, 1, 23, 0, triple, 4)
    half_sweep(sc0, 2, 22, 1, triple, 4)
    half_sweep(sc0, 3, 21, 0, triple, 4)
    half_sweep(sc0, 4, 20, 1, triple, 4)

    totals = jnp.sum(sum_gx.finish(), axis=1, keepdims=True)
    norm_rhs, along, norm_image, second_rhs, second_along, norm_second = (
        totals[at : at + 1, :] for at in range(6)
    )
    alpha = norm_rhs / along
    turned_rest = along - alpha * norm_image - alpha * second_rhs + alpha * alpha * second_along
    turned_norm = norm_image - 2.0 * alpha * second_along + alpha * alpha * norm_second
    omega = turned_rest / turned_norm
    first = jnp.broadcast_to(alpha + omega, (16, LANES))
    other = jnp.broadcast_to(alpha * omega, (16, LANES))

    def combine(x, _):
        at = (x + 4, slice(0, 16), slice(0, LANES))
        out[x] = u0[at] + first * b0[at] - other * c0[at]
        return 0

    lax.fori_loop(0, 16, combine, 0)


def solution(mesh):
    sizes = dict(mesh.shape)

    def per_device(old_slots, old_ids, old_owner, coefficient):
        vmem = pl.BlockSpec(memory_space=pltpu.VMEM)
        far = pl.BlockSpec(memory_space=pltpu.HBM)
        fine, middle, low = (24, 24, 256), (20, 24, 128), (12, 16, 128)
        groups = sizes["gz"]
        sums = sizes["gy"] + sizes["gz"] + sizes["gx"]
        shapes = [
            (512, LANES),
            ("b", 16, 32, LANES),
            ("b", groups * SEND, 32, LANES),
            ("b", groups * SEND, 32, LANES),
            (256, LANES),
            (16, 16, LANES),
            fine,
            middle,
            low,
            (6,) + fine,
            (6,) + middle,
            (6,) + low,
            fine,
            middle,
            low,
            fine,
            middle,
            low,
            fine,
            fine,
            fine,
            middle,
            middle,
            middle,
            low,
            low,
            low,
            middle,
            middle,
            fine,
            fine,
            (8, 16, LANES),
            (12, 24, LANES),
            (12, 16, LANES),
            (2, 12, 24, LANES),
            (3, 16, LANES),
            (3, 2, 9, 16, LANES),
            (3, 2, 8, 8, LANES),
            (3, 2, 8, 8, LANES),
            (3, 2, 2, 4, 8, LANES),
            (3, 8, LANES),
            (3, 9, 4, 8, LANES),
            (3, 2, 9, 8, LANES),
            (2, 3, 9, 8, LANES),
            (3, 8, LANES),
            (sizes["gy"], 8, LANES),
            (sizes["gz"], 8, LANES),
            (sizes["gx"], 8, LANES),
        ]
        scratch = [
            pltpu.VMEM(shape[1:], jnp.bfloat16) if shape[0] == "b" else pltpu.VMEM(shape, F32)
            for shape in shapes
        ]
        dma = pltpu.SemaphoreType.DMA
        scratch += [dma((groups,)), dma((groups,)), dma((208,)), dma((208,))]
        scratch += [dma((sums,)), dma((sums,))]
        scratch += [pltpu.VMEM(old_slots.shape, jnp.bfloat16), pltpu.SMEM(old_ids.shape, jnp.int32)]
        scratch += [pltpu.SMEM(old_owner.shape, jnp.int32), dma((4,))]
        scratch += [pltpu.VMEM((SEND, 32, LANES), jnp.bfloat16), dma((2,))]
        return pl.pallas_call(
            kernel,
            out_shape=jax.ShapeDtypeStruct(coefficient.shape, F32),
            in_specs=[far] * 4,
            out_specs=vmem,
            scratch_shapes=scratch,
            compiler_params=pltpu.CompilerParams(
                collective_id=0, has_side_effects=True, vmem_limit_bytes=67_000_000
            ),
        )(old_slots, old_ids, old_owner, coefficient)

    return jax.shard_map(
        per_device,
        mesh=mesh,
        in_specs=(
            P("gx", "gy", "gz", None),
            P("gx", "gy", "gz"),
            P("gx", "gy", None),
            P("gx", "gy", "gz"),
        ),
        out_specs=P("gx", "gy", "gz"),
        check_vma=False,
    )
```
